512 devices in a mesh: tile: 128 (over y, z, core), shell: 4 (over x).
Axes of the slice: x: 4, y: 8, z: 8, core: 2. Of those that a mesh axis runs over, the one named last changes fastest.
Arguments:
- particles: bfloat16 [4096, 2, 32768], P('tile', None, 'shell'), may hold values from -40 to 40
- projections: bfloat16 [4096, 2, 32768], P('tile', None, 'shell'), may hold values from -6 to 6
- noise_weight: float32 [32768], P('shell'), may hold values from 0.001 to 0.012
- tile_list: int32 [4096, 4], P('tile'), may hold values from 0 to 127, all different within a row; in each aligned block of 32 rows (0 to 31, 32 to 63, ...) at most 2 rows name the same one
- ori_start: int32 [4096, 4], P('tile'), may hold values from 0 to 31
- shifts: int32 [4096, 2], P('tile'), may hold values from -8 to 8
- defocus_bin: int32 [4096], P('tile'), may hold values from 0 to 15
Outputs:
- posterior: float32 [4096, 9, 64], P('tile')
- log_evidence: float32 [4096], P('tile')
The draws below stay inside these ranges and needn't reach their ends.
Inputs may be any that keep to these rules, and one draw needn't show every extreme that they name: `tile_list`: the 4 tiles of one particle differ, and among the particles of one index of tile no tile is named more than 2 times, a count reached.
All inputs are finite; a program needn't handle non-finite values.
Results may differ from the reference program's by a relative error of at most 0.0035.
Values may be sent and summed in bfloat16 or wider, within the bound.
No kernel may reach another device: no remote copies, remote signals or barrier semaphores. Data moves between devices by JAX's collectives and lax.ppermute only.
A program may use at most 128 MiB of HBM per device.

```python
import math
import jax
import jax.numpy as jnp
import numpy as np
from jax import lax

BOX = 256
K = 32768
ORI_DEV = 32
ORI_WIN = 16
N_ORI = 4096
WIN = 4
P_DEV = 32
PARTICLES = 4096
CAP = 2
NBIN = 16
TSIDE = 3
N_TILE = 128


def draw_particles(key, part):
    scale_key = jax.random.fold_in(key, 11)
    noise_key = jax.random.fold_in(key, 12)
    gauss = jax.random.normal(noise_key, (PARTICLES, 2, K), jnp.float32)
    scales = jnp.exp(jax.random.uniform(scale_key, (PARTICLES, 1, 1), jnp.float32, math.log(2.0), math.log(8.0)))
    values = scales * gauss
    return jnp.clip(values, -40.0, 40.0).astype(jnp.bfloat16)


def draw_projections(key, part):
    tile_key = jax.random.fold_in(key, 22)

    def one_tile(tile_index):
        block_key = jax.random.fold_in(tile_key, tile_index)
        raw = jax.random.normal(block_key, (ORI_DEV, 2, K), jnp.float32)
        spread = jnp.sqrt(jnp.mean(raw * raw, axis=(1, 2), keepdims=True))
        return jnp.clip(raw / spread, -6.0, 6.0).astype(jnp.bfloat16)
    tiles = lax.map(one_tile, jnp.arange(N_TILE, dtype=jnp.int32))
    return tiles.reshape(N_ORI, 2, K)


def touch_ends(drawn, rng, least, top_value):
    extent = drawn.shape
    place = [jax.random.randint(jax.random.fold_in(rng, axis), (), 0, extent[axis]) for axis in range(len(extent))]
    drawn = drawn.at[tuple(place)].set(least)
    longest = extent.index(max(extent))
    place[longest] = (place[longest] + 1) % extent[longest]
    return drawn.at[tuple(place)].set(top_value)


def block_levels(own_key, shape, pieces, least, top_value):
    factor_of, own = 1.0, jax.random.fold_in(own_key, 6)
    for axis_at, shards_of in pieces:
        steps = jnp.exp(jax.random.uniform(jax.random.fold_in(own, axis_at), (shards_of,), jnp.float32, least / len(pieces), top_value / len(pieces)))
        factor_of = factor_of * jnp.repeat(steps, shape[axis_at] // shards_of).reshape([-1 if axis == axis_at else 1 for axis in range(len(shape))])
    return factor_of


def routed_block(rng, own, number, rows, amount, top, most, slope):
    ranking = jax.random.permutation(rng, amount)
    crowded, ordinary = shares(amount, rows * top, most, slope, True), shares(amount, rows * top, most, slope, False)
    places = jnp.arange(amount)

    def named(lengths, turn):
        used = int((lengths > 0).sum())
        fixed = max(1, used // 4)
        passed = fixed + (places - fixed + turn * (used - fixed)) % max(1, amount - fixed)
        return jnp.zeros((amount,), jnp.int32).at[ranking[jnp.where(places < fixed, places, passed)]].set(jnp.asarray(lengths, jnp.int32))

    lengths = jnp.where(number % 4 == 0, named(crowded, number // 4), named(ordinary, number - number // 4 - 1))
    mixed = jax.random.permutation(jax.random.fold_in(own, 3), amount)
    giver, receiver = mixed[0:amount // 2 * 2:2], mixed[1:amount // 2 * 2:2]
    slack = jnp.minimum(lengths[giver] - 1, most - lengths[receiver]) // 2
    slack = jnp.where((giver == ranking[0]) | (receiver == ranking[0]) | (lengths[receiver] == 0), 0, jnp.maximum(slack, 0))
    passed = jax.random.randint(jax.random.fold_in(own, 4), (amount // 2,), 0, 1 << 20) % (slack + 1)
    lengths = lengths.at[giver].add(-passed).at[receiver].add(passed)
    items = jnp.searchsorted(jnp.cumsum(lengths), jnp.arange(rows * top), side="right").astype(jnp.int32)
    table = items.reshape(top, rows).T
    table = table[jax.random.permutation(jax.random.fold_in(own, 1), rows)]
    turn = jax.random.randint(jax.random.fold_in(own, 2), (rows, 1), 0, top)
    return jnp.take_along_axis(table, (jnp.arange(top)[None, :] + turn) % top, axis=1)


def shares(amount, total, most, lean, full):
    weights = [(1 << 20) // math.isqrt(grade ** lean) + 1 for grade in range(1, amount + 1)]
    largest = most if full else min(most, max(-(-total // amount), total * weights[0] // sum(weights)))
    least = 1 if total - largest >= amount - 1 else 0
    holding, surplus = [largest] + [least] * (amount - 1), total - largest - least * (amount - 1)
    while surplus > 0:
        free = [i for i in range(1, amount) if holding[i] < largest] or [i for i in range(1, amount) if holding[i] < most]
        pool, left = sum([weights[i] for i in free]), surplus
        for i in free:
            more = min(most - holding[i], max(1, left * weights[i] // pool), surplus)
            holding[i] = holding[i] + more
            surplus = surplus - more
    return np.array(holding)


def setup_inputs(seed: int = 0) -> dict:
    key_of = jax.random.split(jax.random.key(seed), 8)
    particles = draw_particles(jax.random.fold_in(key_of[7], 71), 0)
    projections = draw_projections(jax.random.fold_in(key_of[7], 71), 0)
    noise_weight = jnp.clip(jnp.exp(math.log(0.012) - 2.4849066 * jax.random.uniform(key_of[2], (K,), jnp.float32) ** block_levels(key_of[2], (K,), ((0, 4),), -0.2, 0.2)), 0.001, 0.012)
    tile_list_keys = jax.random.split(jax.random.fold_in(key_of[3], 1), PARTICLES // P_DEV)
    tile_list_turns = jax.random.permutation(jax.random.fold_in(key_of[3], 3), PARTICLES // P_DEV)
    tile_list = jax.vmap(lambda own, number: routed_block(jax.random.fold_in(key_of[3], 2), own, number, P_DEV, N_TILE, WIN, CAP, 2))(tile_list_keys, tile_list_turns).reshape((PARTICLES, WIN))
    ori_start = touch_ends(jax.random.randint(key_of[4], (PARTICLES, WIN), 0, ORI_DEV), jax.random.fold_in(key_of[4], 1), 0, ORI_DEV - 1).astype(jnp.int32)
    shifts = touch_ends(jax.random.randint(key_of[5], (PARTICLES, 2), -8, 9), jax.random.fold_in(key_of[5], 1), -8, 8).astype(jnp.int32)
    defocus_bin = touch_ends(jax.random.randint(key_of[6], (PARTICLES,), 0, NBIN), jax.random.fold_in(key_of[6], 1), 0, NBIN - 1).astype(jnp.int32)
    return {"particles": particles, "projections": projections, "noise_weight": noise_weight, "tile_list": tile_list, "ori_start": ori_start, "shifts": shifts, "defocus_bin": defocus_bin}


wave_length = 0.0197
aberration = 27000000.0
amplitude = 0.1
b_factor = 20.0
defocus_base = 5000.0
defocus_step = 500.0

def frequencies(first_index, span_count):
    flat_index = first_index + jnp.arange(span_count, dtype=jnp.int32)
    freq_x = flat_index // BOX
    freq_y = flat_index % BOX - BOX // 2
    return (freq_x, freq_y)

def ctf_table(freq_x, freq_y, bins_count):
    scaled_x = freq_x.astype(jnp.float32) / BOX
    scaled_y = freq_y.astype(jnp.float32) / BOX
    radius_sq = scaled_x * scaled_x + scaled_y * scaled_y
    defocus = defocus_base + defocus_step * jnp.arange(bins_count, dtype=jnp.float32)[:, None]
    aberr_phase = math.pi * wave_length * defocus * radius_sq[None, :] - 0.5 * math.pi * aberration * wave_length ** 3 * radius_sq[None, :] ** 2
    envelope = jnp.exp(-0.25 * b_factor * radius_sq)[None, :]
    return -(math.sqrt(1.0 - amplitude ** 2) * jnp.sin(aberr_phase) + amplitude * jnp.cos(aberr_phase)) * envelope

def rotation(freq_x, freq_y, mult_x, mult_y):
    phase_turns = jnp.mod(freq_x * mult_x + freq_y * mult_y, BOX)
    angles = phase_turns.astype(jnp.float32) * (2.0 * math.pi / BOX)
    return (jnp.cos(angles), jnp.sin(angles))

def pick_rows(bin_index, lookup):
    one_hot = (bin_index[:, None] == jnp.arange(lookup.shape[0], dtype=jnp.int32)[None, :]).astype(jnp.float32)
    return jnp.dot(one_hot, lookup, precision=lax.Precision.HIGHEST, preferred_element_type=jnp.float32)

def prepare(particles, weight, ctf_rows, shifts, freq_x, freq_y):
    values = particles.astype(jnp.float32)
    real_part = values[:, 0]
    imag_part = values[:, 1]
    cosine, sine_value = rotation(freq_x[None, :], freq_y[None, :], shifts[:, 0:1], shifts[:, 1:2])
    moved_real = real_part * cosine + imag_part * sine_value
    moved_imag = imag_part * cosine - real_part * sine_value
    factor = weight[None, :] * ctf_rows
    weighted = jnp.stack([factor * moved_real, factor * moved_imag], axis=1).astype(jnp.bfloat16)
    energy = lax.optimization_barrier(jnp.sum(weight[None, :] * (real_part * real_part + imag_part * imag_part), axis=1))
    return (weighted, energy)

def shifted_tables(projections, freq_x, freq_y):
    offsets = jnp.arange(TSIDE, dtype=jnp.int32) - TSIDE // 2
    mult_x = jnp.repeat(offsets, TSIDE)[:, None]
    mult_y = jnp.tile(offsets, TSIDE)[:, None]
    cosine, sine_value = rotation(freq_x[None, :], freq_y[None, :], mult_x, mult_y)
    cosine = cosine[:, None, :]
    sine_value = sine_value[:, None, :]
    proj_real = projections[:, 0].astype(jnp.float32)[None, :, :]
    proj_imag = projections[:, 1].astype(jnp.float32)[None, :, :]
    moved_real = proj_real * cosine - proj_imag * sine_value
    moved_imag = proj_imag * cosine + proj_real * sine_value
    stacked = jnp.stack([moved_real, moved_imag], axis=2).astype(jnp.bfloat16)
    return stacked.reshape(TSIDE * TSIDE * projections.shape[0], -1)

def slot_scores(slot_rows, bin_index, projections, weight, ctf, freq_x, freq_y):
    orient_count = projections.shape[0]
    lookup = shifted_tables(projections, freq_x, freq_y)
    cross_term = lax.dot_general(slot_rows, lookup, (((1,), (1,)), ((), ())), preferred_element_type=jnp.float32)
    cross_term = cross_term.reshape(slot_rows.shape[0], TSIDE * TSIDE, orient_count)
    proj_values = projections.astype(jnp.float32)
    magnitude = proj_values[:, 0] * proj_values[:, 0] + proj_values[:, 1] * proj_values[:, 1]
    weighted_ctf = weight[None, :] * ctf * ctf
    power = lax.dot_general(weighted_ctf, magnitude, (((1,), (1,)), ((), ())), precision=lax.Precision.HIGHEST, preferred_element_type=jnp.float32)
    power_rows = pick_rows(bin_index, power)
    return cross_term - 0.5 * power_rows[:, None, :]

def window(scores, starts, orient_count):
    orient_index = jnp.mod(starts[:, None] + jnp.arange(orient_count // 2, dtype=jnp.int32)[None, :], orient_count)
    return jnp.take_along_axis(scores, orient_index[:, None, :], axis=2)

def slot_layout(tile_ids, tile_count, capacity):
    positions = jnp.arange(tile_ids.shape[0], dtype=jnp.int32)
    earlier_same = (tile_ids[:, None] == tile_ids[None, :]) & (positions[None, :] < positions[:, None])
    slot_rank = lax.optimization_barrier(jnp.sum(earlier_same.astype(jnp.int32), axis=1))
    slot_index = tile_ids * capacity + slot_rank
    matches = slot_index[None, :] == jnp.arange(tile_count * capacity, dtype=jnp.int32)[:, None]
    slot_owner = lax.optimization_barrier(jnp.sum(jnp.where(matches, positions[None, :] + 1, 0), axis=1)) - 1
    return (slot_index, slot_owner)

def finish(scores, energy_sum):
    scored = scores - 0.5 * energy_sum[:, None, None]
    row_peak = lax.optimization_barrier(jnp.max(scored, axis=(1, 2)))
    log_total = row_peak + jnp.log(lax.optimization_barrier(jnp.sum(jnp.exp(scored - row_peak[:, None, None]), axis=(1, 2))))
    posterior = jnp.exp(scored - log_total[:, None, None])
    return (posterior, log_total)

def reference(particles, projections, noise_weight, tile_list, ori_start, shifts, defocus_bin):
    capacity = CAP
    freq_x, freq_y = frequencies(0, K)
    ctf = ctf_table(freq_x, freq_y, NBIN)

    def prep_block(block_index):
        first = block_index * P_DEV
        block_particles = lax.dynamic_slice_in_dim(particles, first, P_DEV, 0)
        block_shifts = lax.dynamic_slice_in_dim(shifts, first, P_DEV, 0)
        block_bins = lax.dynamic_slice_in_dim(defocus_bin, first, P_DEV, 0)
        return prepare(block_particles, noise_weight, pick_rows(block_bins, ctf), block_shifts, freq_x, freq_y)
    weighted, energy = lax.map(prep_block, jnp.arange(N_TILE, dtype=jnp.int32))
    weighted = weighted.reshape(PARTICLES, 2 * K)
    energy = energy.reshape(PARTICLES)
    block_tiles = tile_list.reshape(N_TILE, P_DEV * WIN)
    slots_all, owners_all = jax.vmap(lambda tile_ids: slot_layout(tile_ids, N_TILE, capacity))(block_tiles)
    starts_flat = ori_start.reshape(-1)

    def score_tile(tile_index):
        slot_owner = lax.dynamic_slice_in_dim(owners_all, tile_index * capacity, capacity, 1)
        source_index = jnp.arange(N_TILE, dtype=jnp.int32)[:, None]
        item_index = (source_index * (P_DEV * WIN) + jnp.maximum(slot_owner, 0)).reshape(-1)
        particle = item_index // WIN
        occupied = (slot_owner >= 0).reshape(-1)
        slot_rows = jnp.where(occupied[:, None], weighted[particle], jnp.zeros((), weighted.dtype))
        tile_proj = lax.dynamic_slice_in_dim(projections, tile_index * ORI_DEV, ORI_DEV, 0)
        partial_value = slot_scores(slot_rows, defocus_bin[particle], tile_proj, noise_weight, ctf, freq_x, freq_y)
        chosen = window(partial_value, starts_flat[item_index], ORI_DEV)
        return chosen.reshape(N_TILE, capacity, TSIDE * TSIDE, ORI_WIN)
    results = lax.map(score_tile, jnp.arange(N_TILE, dtype=jnp.int32))
    tiles_flat = tile_list.reshape(-1)
    source_of = jnp.arange(PARTICLES * WIN, dtype=jnp.int32) // (P_DEV * WIN)
    slot_rank = slots_all.reshape(-1) - tiles_flat * capacity
    returned = results[tiles_flat, source_of, slot_rank]
    returned = returned.reshape(PARTICLES, WIN, TSIDE * TSIDE, ORI_WIN)
    scores = jnp.transpose(returned, (0, 2, 1, 3)).reshape(PARTICLES, TSIDE * TSIDE, WIN * ORI_WIN)
    return finish(scores, energy)
```

```python
import functools
import math

import jax
import jax.numpy as jnp
from jax import lax
from jax.experimental import pallas as pl
from jax.experimental.pallas import tpu as pltpu
from jax.sharding import Mesh
from jax.sharding import PartitionSpec as P

BOX = 256
NBIN = 16
TSIDE = 3
NT = TSIDE * TSIDE
TILE = ("tile_0", "tile_1", "tile_2")

wave_length = 0.0197
aberration = 27000000.0
amplitude = 0.1
b_factor = 20.0
defocus_base = 5000.0
defocus_step = 500.0

META = 128
CHUNK = 512
PAIRS = ((5, 3, 0, 1), (7, 1, 1, 0), (8, 0, 1, 1), (6, 2, 1, -1))


def ring_offsets(n):
    offs = [0]
    for s in range(1, n // 2):
        offs += [s, -s]
    return offs + [n // 2]


def frequencies(first_index, span_count):
    flat_index = first_index + jnp.arange(span_count, dtype=jnp.int32)
    freq_x = flat_index // BOX
    freq_y = flat_index % BOX - BOX // 2
    return (freq_x, freq_y)


def ctf_table(freq_x, freq_y, bins_count):
    scaled_x = freq_x.astype(jnp.float32) / BOX
    scaled_y = freq_y.astype(jnp.float32) / BOX
    radius_sq = scaled_x * scaled_x + scaled_y * scaled_y
    defocus = defocus_base + defocus_step * jnp.arange(bins_count, dtype=jnp.float32)[:, None]
    aberr_phase = (
        math.pi * wave_length * defocus * radius_sq[None, :]
        - 0.5 * math.pi * aberration * wave_length**3 * radius_sq[None, :] ** 2
    )
    envelope = jnp.exp(-0.25 * b_factor * radius_sq)[None, :]
    return (
        -(math.sqrt(1.0 - amplitude**2) * jnp.sin(aberr_phase) + amplitude * jnp.cos(aberr_phase))
        * envelope
    )


def turn(m):
    angles = jnp.mod(m, BOX).astype(jnp.float32) * (2.0 * math.pi / BOX)
    return (jnp.cos(angles), jnp.sin(angles))


def split3(v):
    hi = v.astype(jnp.bfloat16)
    rest = v - hi.astype(jnp.float32)
    mid = rest.astype(jnp.bfloat16)
    lo = (rest - mid.astype(jnp.float32)).astype(jnp.bfloat16)
    return hi, mid, lo


NT_DIMS = (((1,), (1,)), ((), ()))


def prep_kernel(c_ref, xr, xi, qr, qi, w, ctf, binc, cx, sx, cy, sy, meta, out, energy, wc2_s, mag_s):
    n, width = xr.shape
    half = width // 2
    c = c_ref[0]
    bins = binc[...]
    acc = jnp.zeros((n, BOX), jnp.float32)
    cyv = cy[...]
    syv = sy[...]
    for g in range(width // BOX):
        sl = pl.ds(g * BOX, BOX)
        wv = w[:, sl]
        table = ctf[:, sl]
        wc2_s[:, sl] = wv * table * table
        rows = jnp.zeros((n, BOX), jnp.float32)
        for b in range(NBIN):
            rows = jnp.where(bins == b, table[b : b + 1, :], rows)
        re = xr[:, sl].astype(jnp.float32)
        im = xi[:, sl].astype(jnp.float32)
        cxv = cx[:, g : g + 1]
        sxv = sx[:, g : g + 1]
        co = cxv * cyv - sxv * syv
        si = sxv * cyv + cxv * syv
        factor = wv * rows
        h = (g * BOX) // half
        at = g * BOX - h * half
        place = (at // CHUNK) * 2 * CHUNK + at % CHUNK
        d = (h + c) % 2
        out[d, 0:n, pl.ds(place, BOX)] = (factor * (re * co + im * si)).astype(jnp.bfloat16)
        out[d, 0:n, pl.ds(place + CHUNK, BOX)] = (factor * (im * co - re * si)).astype(jnp.bfloat16)
        acc = acc + wv * (re * re + im * im)
        pr = qr[:, sl]
        pi = qi[:, sl]
        out[d, n : 2 * n, pl.ds(place, BOX)] = pr
        out[d, n : 2 * n, pl.ds(place + CHUNK, BOX)] = pi
        prf = pr.astype(jnp.float32)
        pif = pi.astype(jnp.float32)
        mag_s[:, sl] = prf * prf + pif * pif
    energy[...] = jnp.broadcast_to(jnp.sum(acc, axis=1, keepdims=True), (n, META))
    power = lax.dot_general(
        mag_s[...], wc2_s[...], NT_DIMS, precision=lax.Precision.HIGHEST, preferred_element_type=jnp.float32
    )
    lane = lax.broadcasted_iota(jnp.int32, (NBIN, META), 1)
    row = lax.broadcasted_iota(jnp.int32, (NBIN, META), 0)
    placed = jnp.zeros((n, META), jnp.float32)
    for k, part in enumerate(split3(power)):
        spot = jnp.where(lane == row + k * NBIN, 1.0, 0.0).astype(jnp.bfloat16)
        placed = placed + jnp.dot(part, spot, preferred_element_type=jnp.float32)
    for d in range(2):
        out[d, 0:n, pl.ds(width, META)] = meta[...]
        out[d, n : 2 * n, pl.ds(width, META)] = placed.astype(jnp.bfloat16)


def prepare(c, xr, xi, qr, qi, w, ctf, binc, cx, sx, cy, sy, meta):
    n, width = xr.shape
    vm = pl.BlockSpec(memory_space=pltpu.VMEM)
    return pl.pallas_call(
        prep_kernel,
        out_shape=(
            jax.ShapeDtypeStruct((2, 2 * n, width + META), jnp.bfloat16),
            jax.ShapeDtypeStruct((n, META), jnp.float32),
        ),
        in_specs=[pl.BlockSpec(memory_space=pltpu.SMEM)] + [vm] * 12,
        out_specs=(vm, vm),
        scratch_shapes=[pltpu.VMEM((NBIN, width), jnp.float32), pltpu.VMEM((n, width), jnp.float32)],
        name="prep",
    )(c, xr, xi, qr, qi, w, ctf, binc, cx, sx, cy, sy, meta)


def score_kernel(n_y, n_z, ids, *refs):
    yb = refs[: n_y + 1]
    zb = refs[n_y + 1 : n_y + n_z + 2]
    tables, meta_y, meta_z, out, part_s, proj_s, rot_s, acc, w_s = refs[n_y + n_z + 2 :]
    step = pl.program_id(0)
    steps = pl.num_programs(0)
    rows = yb[0].shape[0]
    half_rows = rows // 2
    np_ = n_y * rows
    offs_y = ring_offsets(n_y)
    offs_z = ring_offsets(n_z)

    for k in range(n_y - 1):
        part_s[k * rows : (k + 1) * rows, :] = yb[k][...]
    part_s[(n_y - 1) * rows : (n_y - 1) * rows + half_rows, :] = yb[n_y - 1][...]
    part_s[(n_y - 1) * rows + half_rows : n_y * rows, :] = yb[n_y][...]
    for k in range(n_z - 1):
        proj_s[k] = zb[k][...]
    proj_s[n_z - 1, 0:half_rows, :] = zb[n_z - 1][...]
    proj_s[n_z - 1, half_rows:rows, :] = zb[n_z][...]

    def rotate(b, slot):
        for s in range(rows // 16):
            sl = slice(s * 16, s * 16 + 16)
            for q in range(CHUNK // 256):
                la = slice(q * 256, q * 256 + 256)
                lb = slice(CHUNK + q * 256, CHUNK + q * 256 + 256)
                reb = proj_s[b, sl, la]
                imb = proj_s[b, sl, lb]
                re = reb.astype(jnp.float32)
                im = imb.astype(jnp.float32)
                base = 4 * rows + s * 16
                rot_s[slot, base : base + 16, la] = reb
                rot_s[slot, base : base + 16, lb] = imb
                for k, (t1, t2, _, _) in enumerate(PAIRS):
                    co = tables[k : k + 1, la]
                    si = tables[4 + k : 5 + k, la]
                    rc = re * co
                    is_ = im * si
                    ic = im * co
                    rs = re * si
                    b1 = t1 * rows + s * 16
                    b2 = t2 * rows + s * 16
                    rot_s[slot, b1 : b1 + 16, la] = (rc - is_).astype(jnp.bfloat16)
                    rot_s[slot, b1 : b1 + 16, lb] = (ic + rs).astype(jnp.bfloat16)
                    rot_s[slot, b2 : b2 + 16, la] = (rc + is_).astype(jnp.bfloat16)
                    rot_s[slot, b2 : b2 + 16, lb] = (ic - rs).astype(jnp.bfloat16)

    @pl.when(step == 0)
    def _():
        acc[...] = jnp.zeros_like(acc)

    rotate(0, 0)

    def body(b, carry):
        acc[b] += lax.dot_general(
            rot_s[b % 2], part_s[...], NT_DIMS, preferred_element_type=jnp.float32
        )
        rotate(jnp.minimum(b + 1, n_z - 1), (b + 1) % 2)
        return carry

    lax.fori_loop(0, n_z, body, 0)

    @pl.when(step == steps - 1)
    def _():
        my_y = ids[0]
        my_z = ids[1]
        my_c = ids[2]
        info = jnp.transpose(meta_y[...].astype(jnp.float32)).astype(jnp.int32)
        bins = info[8:9, :]
        r = lax.broadcasted_iota(jnp.int32, (META, np_), 0)
        spot = jnp.where((r % NBIN == bins) & (r < 3 * NBIN), -0.25, 0.0).astype(jnp.bfloat16)
        power = jnp.dot(meta_z[...], spot, preferred_element_type=jnp.float32)
        for lt in range(np_ // 128):
            la = slice(lt * 128, lt * 128 + 128)
            for t in range(NT):
                sums = [jnp.zeros((half_rows, 128), jnp.float32) for _ in range(4)]
                for k in range(n_z):
                    z_abs = (my_z - offs_z[k] + n_z) % n_z
                    for u in range(2):
                        tile = (my_y * n_z + z_abs) * 2 + (my_c + u) % 2
                        lo = t * rows + u * half_rows
                        val = acc[k, lo : lo + half_rows, la]
                        lo = k * rows + u * half_rows
                        val = val + power[lo : lo + half_rows, la]
                        for j in range(4):
                            sums[j] = jnp.where(info[j : j + 1, la] // 2 == tile, val, sums[j])
                for j in range(4):
                    x = sums[j]
                    start = info[4 + j : 5 + j, la]
                    for bit in (16, 8, 4, 2, 1):
                        x = jnp.where((start & bit) != 0, pltpu.roll(x, half_rows - bit, 0), x)
                    w_s[j, t * 16 : t * 16 + 16, la] = x[0:16]
        lane = lax.broadcasted_iota(jnp.int32, (1, np_), 1)
        k_of = lane // rows
        c_of = ((lane // half_rows) + my_c) % 2
        y_of = jnp.zeros((1, np_), jnp.int32)
        for k in range(n_y):
            y_of = jnp.where(k_of == k, (my_y - offs_y[k] + n_y) % n_y, y_of)
        per_row = 4 * n_z
        n_slots = out.shape[0]
        slot_row = lax.broadcasted_iota(jnp.int32, (n_slots, np_), 0)
        total = jnp.zeros(out.shape, jnp.float32)
        for j in range(4):
            local = info[j : j + 1, :] - my_y * per_row
            fits = (local >= 0) & (local < per_row)
            slot = jnp.where(fits, (y_of * 2 + c_of) * per_row + local, -1)
            pick = jnp.where(slot_row == slot, 1.0, 0.0).astype(jnp.bfloat16)
            for piece in split3(w_s[j]):
                total = total + lax.dot_general(pick, piece, NT_DIMS, preferred_element_type=jnp.float32)
        out[...] = total


def score(ids, y_blocks, z_blocks, tables, meta_y, meta_z):
    n_y = len(y_blocks) - 1
    n_z = len(z_blocks) - 1
    rows = y_blocks[0].shape[0]
    width = y_blocks[0].shape[1] - META
    steps = width // (2 * CHUNK)
    span = 2 * CHUNK
    blocks = [
        pl.BlockSpec((a.shape[0], span), lambda i, s: (0, i)) for a in list(y_blocks) + list(z_blocks)
    ]
    full = lambda a: pl.BlockSpec(a.shape, lambda i, s: (0, 0))
    n_slots = 2 * n_y * 4 * n_z
    flops = 2 * NT * rows * n_z * rows * n_y * width
    return pl.pallas_call(
        functools.partial(score_kernel, n_y, n_z),
        out_shape=jax.ShapeDtypeStruct((n_slots, NT * 16), jnp.float32),
        grid_spec=pltpu.PrefetchScalarGridSpec(
            num_scalar_prefetch=1,
            grid=(steps,),
            in_specs=blocks
            + [pl.BlockSpec((8, CHUNK), lambda i, s: (0, i)), full(meta_y), full(meta_z)],
            out_specs=pl.BlockSpec((n_slots, NT * 16), lambda i, s: (0, 0)),
            scratch_shapes=[
                pltpu.VMEM((n_y * rows, span), jnp.bfloat16),
                pltpu.VMEM((n_z, rows, span), jnp.bfloat16),
                pltpu.VMEM((2, NT * rows, span), jnp.bfloat16),
                pltpu.VMEM((n_z, NT * rows, n_y * rows), jnp.float32),
                pltpu.VMEM((4, NT * 16, n_y * rows), jnp.float32),
            ],
        ),
        compiler_params=pltpu.CompilerParams(
            dimension_semantics=("arbitrary",), vmem_limit_bytes=60 * 1024 * 1024
        ),
        cost_estimate=pl.CostEstimate(flops=flops, transcendentals=0, bytes_accessed=17 * 1024 * 1024),
        name="score",
    )(ids, *y_blocks, *z_blocks, tables, meta_y, meta_z)


def both_rings(a, axis_a, b, axis_b):
    found = {0: [a], 1: [b]}
    axes = (axis_a, axis_b)
    sizes = [lax.axis_size(x) for x in axes]
    ahead = [a, b]
    back = [a, b]

    def shift(v, k, d):
        n = sizes[k]
        return lax.ppermute(v, axes[k], [(i, (i + d) % n) for i in range(n)])

    for s in range(1, max(sizes) // 2 + 1):
        for k in range(2):
            n = sizes[k]
            if s < n // 2:
                ahead[k] = shift(ahead[k], k, 1)
                back[k] = shift(back[k], k, -1)
                found[k] += [ahead[k], back[k]]
            elif s == n // 2:
                h = a.shape[0] // 2
                found[k] += [shift(ahead[k][:h], k, 1), shift(back[k][h:], k, -1)]
    return found[0], found[1]


def slot_rank(tile_ids):
    positions = jnp.arange(tile_ids.shape[0], dtype=jnp.int32)
    earlier_same = (tile_ids[:, None] == tile_ids[None, :]) & (
        positions[None, :] < positions[:, None]
    )
    return jnp.sum(earlier_same.astype(jnp.int32), axis=1)


def finish(scored):
    row_peak = jnp.max(scored, axis=(1, 2))
    log_total = row_peak + jnp.log(jnp.sum(jnp.exp(scored - row_peak[:, None, None]), axis=(1, 2)))
    posterior = jnp.exp(scored - log_total[:, None, None])
    return (posterior, log_total)


def per_device(particles, projections, noise_weight, tile_list, ori_start, shifts, defocus_bin):
    band = lax.axis_index("shell")
    my_y = lax.axis_index(TILE[0])
    my_z = lax.axis_index(TILE[1])
    my_c = lax.axis_index(TILE[2])
    count, _, width = particles.shape
    windows = tile_list.shape[1]
    half = width // 2
    freq_x, freq_y = frequencies(band * width, width)
    ctf = ctf_table(freq_x, freq_y, NBIN)
    first_x = (band * width) // BOX
    span_x = first_x + jnp.arange(width // BOX, dtype=jnp.int32)
    span_y = jnp.arange(BOX, dtype=jnp.int32) - BOX // 2
    cx, sx = turn(span_x[None, :] * shifts[:, 0:1])
    cy, sy = turn(span_y[None, :] * shifts[:, 1:2])
    key = tile_list * 2 + slot_rank(tile_list.reshape(-1)).reshape(count, windows)
    meta = jnp.concatenate([key, ori_start, defocus_bin[:, None]], axis=1)
    meta = jnp.pad(meta, ((0, 0), (0, META - meta.shape[1]))).astype(jnp.bfloat16)
    sides, energy = prepare(
        my_c.reshape(1).astype(jnp.int32),
        particles[:, 0],
        particles[:, 1],
        projections[:, 0],
        projections[:, 1],
        noise_weight[None, :],
        ctf,
        defocus_bin[:, None],
        cx,
        sx,
        cy,
        sy,
        meta,
    )
    kept = sides[0]
    got = lax.ppermute(sides[1], TILE[2], [(0, 1), (1, 0)])
    y_own = jnp.concatenate([kept[:count], got[:count]], axis=0)
    z_own = jnp.concatenate([kept[count:], got[count:]], axis=0)
    y_blocks, z_blocks = both_rings(y_own, TILE[0], z_own, TILE[1])
    mult = jnp.array([[a, b] for _, _, a, b in PAIRS], jnp.int32)
    fx = lax.dynamic_slice_in_dim(freq_x, my_c * half, half)
    fy = lax.dynamic_slice_in_dim(freq_y, my_c * half, half)
    co, si = turn(mult[:, 0:1] * fx[None, :] + mult[:, 1:2] * fy[None, :])
    tables = jnp.concatenate([co, si], axis=0)
    meta_y = jnp.concatenate([b[:, half * 2 :] for b in y_blocks], axis=0)
    meta_z = jnp.concatenate([b[:, half * 2 :] for b in z_blocks], axis=0)
    ids = jnp.stack([my_y, my_z, my_c]).astype(jnp.int32)
    slots = score(ids, y_blocks, z_blocks, tables, meta_y, meta_z)
    n_y = lax.axis_size(TILE[0])
    slots = slots.reshape(2 * n_y, -1, NT * 16)
    slots = lax.all_to_all(slots, (TILE[0], TILE[2]), split_axis=0, concat_axis=0, tiled=True)
    slots = jnp.sum(slots.reshape(n_y, 2, -1, NT * 16), axis=1).reshape(-1, NT * 16)
    items = jnp.take(slots, key.reshape(-1), axis=0)
    items = items.reshape(count, windows * NT * 16) - 0.5 * energy[:, 0:1]
    n_x = lax.axis_size("shell")
    copies = jnp.broadcast_to(items, (n_x, *items.shape))
    items = jnp.sum(lax.all_to_all(copies, "shell", split_axis=0, concat_axis=0, tiled=True), axis=0)
    scores = items.reshape(count, windows, NT, 16).transpose(0, 2, 1, 3).reshape(count, NT, windows * 16)
    return finish(scores)


def solution(mesh):
    split = Mesh(
        mesh.devices.reshape(8, 8, 2, mesh.shape["shell"]), ("tile_0", "tile_1", "tile_2", "shell")
    )
    in_specs = (
        P(TILE, None, "shell"),
        P(TILE, None, "shell"),
        P("shell"),
        P(TILE, None),
        P(TILE, None),
        P(TILE, None),
        P(TILE),
    )
    out_specs = (P(TILE, None, None), P(TILE))
    return jax.shard_map(
        per_device, mesh=split, in_specs=in_specs, out_specs=out_specs, check_vma=False
    )
```

```python
import functools
import math

import jax
import jax.numpy as jnp
from jax import lax
from jax.experimental import pallas as pl
from jax.experimental.pallas import tpu as pltpu
from jax.sharding import Mesh
from jax.sharding import PartitionSpec as P

BOX = 256
NBIN = 16
TSIDE = 3
NT = TSIDE * TSIDE
TILE = ("tile_0", "tile_1", "tile_2")

wave_length = 0.0197
aberration = 27000000.0
amplitude = 0.1
b_factor = 20.0
defocus_base = 5000.0
defocus_step = 500.0

META = 128
CHUNK = 1024
PAIRS = ((5, 3, 0, 1), (7, 1, 1, 0), (8, 0, 1, 1), (6, 2, 1, -1))


def ring_offsets(n):
    offs = [0]
    for s in range(1, n // 2):
        offs += [s, -s]
    return offs + [n // 2]


def frequencies(first_index, span_count):
    flat_index = first_index + jnp.arange(span_count, dtype=jnp.int32)
    freq_x = flat_index // BOX
    freq_y = flat_index % BOX - BOX // 2
    return (freq_x, freq_y)


def ctf_table(freq_x, freq_y, bins_count):
    scaled_x = freq_x.astype(jnp.float32) / BOX
    scaled_y = freq_y.astype(jnp.float32) / BOX
    radius_sq = scaled_x * scaled_x + scaled_y * scaled_y
    defocus = defocus_base + defocus_step * jnp.arange(bins_count, dtype=jnp.float32)[:, None]
    aberr_phase = (
        math.pi * wave_length * defocus * radius_sq[None, :]
        - 0.5 * math.pi * aberration * wave_length**3 * radius_sq[None, :] ** 2
    )
    envelope = jnp.exp(-0.25 * b_factor * radius_sq)[None, :]
    return (
        -(math.sqrt(1.0 - amplitude**2) * jnp.sin(aberr_phase) + amplitude * jnp.cos(aberr_phase))
        * envelope
    )


def turn(m):
    angles = jnp.mod(m, BOX).astype(jnp.float32) * (2.0 * math.pi / BOX)
    return (jnp.cos(angles), jnp.sin(angles))


def split3(v):
    hi = v.astype(jnp.bfloat16)
    rest = v - hi.astype(jnp.float32)
    mid = rest.astype(jnp.bfloat16)
    lo = (rest - mid.astype(jnp.float32)).astype(jnp.bfloat16)
    return hi, mid, lo


NT_DIMS = (((1,), (1,)), ((), ()))


def prep_kernel(c_ref, xr, xi, qr, qi, w, ctf, binc, cx, sx, cy, sy, meta, y_keep, z_keep, send, energy, wc2_s, mag_s):
    n, width = xr.shape
    half = width // 2
    c = c_ref[0]
    bins = binc[...]
    acc = jnp.zeros((n, BOX), jnp.float32)
    cyv = cy[...]
    syv = sy[...]

    def put(mine, place, wr, wi, pr, pi):
        a = pl.ds(place, BOX)
        b = pl.ds(place + CHUNK, BOX)

        @pl.when(mine)
        def _():
            y_keep[:, a] = wr
            y_keep[:, b] = wi
            z_keep[:, a] = pr
            z_keep[:, b] = pi

        @pl.when(jnp.logical_not(mine))
        def _():
            send[0:n, a] = wr
            send[0:n, b] = wi
            send[n : 2 * n, a] = pr
            send[n : 2 * n, b] = pi

    for g in range(width // BOX):
        sl = pl.ds(g * BOX, BOX)
        wv = w[:, sl]
        table = ctf[:, sl]
        wc2_s[:, sl] = wv * table * table
        rows = jnp.zeros((n, BOX), jnp.float32)
        for b in range(NBIN):
            rows = jnp.where(bins == b, table[b : b + 1, :], rows)
        re = xr[:, sl].astype(jnp.float32)
        im = xi[:, sl].astype(jnp.float32)
        cxv = cx[:, g : g + 1]
        sxv = sx[:, g : g + 1]
        co = cxv * cyv - sxv * syv
        si = sxv * cyv + cxv * syv
        factor = wv * rows
        h = (g * BOX) // half
        at = g * BOX - h * half
        place = (at // CHUNK) * 2 * CHUNK + at % CHUNK
        wr = (factor * (re * co + im * si)).astype(jnp.bfloat16)
        wi = (factor * (im * co - re * si)).astype(jnp.bfloat16)
        acc = acc + wv * (re * re + im * im)
        pr = qr[:, sl]
        pi = qi[:, sl]
        put(c == h, place, wr, wi, pr, pi)
        prf = pr.astype(jnp.float32)
        pif = pi.astype(jnp.float32)
        mag_s[:, sl] = prf * prf + pif * pif
    energy[...] = jnp.broadcast_to(jnp.sum(acc, axis=1, keepdims=True), (n, META))
    power = lax.dot_general(
        mag_s[...], wc2_s[...], NT_DIMS, precision=lax.Precision.HIGHEST, preferred_element_type=jnp.float32
    )
    lane = lax.broadcasted_iota(jnp.int32, (NBIN, META), 1)
    row = lax.broadcasted_iota(jnp.int32, (NBIN, META), 0)
    placed = jnp.zeros((n, META), jnp.float32)
    for k, part in enumerate(split3(power)):
        spot = jnp.where(lane == row + k * NBIN, 1.0, 0.0).astype(jnp.bfloat16)
        placed = placed + jnp.dot(part, spot, preferred_element_type=jnp.float32)
    tail = pl.ds(width, META)
    placed = placed.astype(jnp.bfloat16)
    y_keep[:, tail] = meta[...]
    z_keep[:, tail] = placed
    send[0:n, tail] = meta[...]
    send[n : 2 * n, tail] = placed


def prepare(c, xr, xi, qr, qi, w, ctf, binc, cx, sx, cy, sy, meta):
    n, width = xr.shape
    vm = pl.BlockSpec(memory_space=pltpu.VMEM)
    return pl.pallas_call(
        prep_kernel,
        out_shape=(
            jax.ShapeDtypeStruct((n, width + META), jnp.bfloat16),
            jax.ShapeDtypeStruct((n, width + META), jnp.bfloat16),
            jax.ShapeDtypeStruct((2 * n, width + META), jnp.bfloat16),
            jax.ShapeDtypeStruct((n, META), jnp.float32),
        ),
        in_specs=[pl.BlockSpec(memory_space=pltpu.SMEM)] + [vm] * 12,
        out_specs=(vm, vm, vm, vm),
        scratch_shapes=[pltpu.VMEM((NBIN, width), jnp.float32), pltpu.VMEM((n, width), jnp.float32)],
        name="prep",
    )(c, xr, xi, qr, qi, w, ctf, binc, cx, sx, cy, sy, meta)


def score_kernel(n_y, n_z, ids, *refs):
    it = iter(refs)
    take = lambda n: [next(it) for _ in range(n)]
    yb = take(2 * n_y)
    zb = take(2 * n_z)
    z_next = take(4)
    tables, tables_next = take(2)
    meta_y = take(2 * n_y)
    meta_z = take(2 * n_z)
    out, part_s, proj_s, tab_s, rot_s, acc, w_s = take(7)
    step = pl.program_id(0)
    steps = pl.num_programs(0)
    piece = yb[0].shape[0]
    rows = 2 * piece
    wide = 2 * rows
    pairs = n_z // 2
    np_ = n_y * rows
    offs_y = ring_offsets(n_y)
    offs_z = ring_offsets(n_z)

    for k, ref in enumerate(yb):
        part_s[k * piece : (k + 1) * piece, :] = ref[...]
    for k, ref in enumerate(zb + z_next):
        proj_s[k // 4, (k % 4) * piece : (k % 4 + 1) * piece, :] = ref[...]
    tab_s[0] = tables[...]
    tab_s[1] = tables_next[...]

    def rotate(b, slot, later):
        for s in range(wide // 16):
            sl = slice(s * 16, s * 16 + 16)
            for q in range(CHUNK // 256):
                la = slice(q * 256, q * 256 + 256)
                lb = slice(CHUNK + q * 256, CHUNK + q * 256 + 256)
                reb = proj_s[b, sl, la]
                imb = proj_s[b, sl, lb]
                re = reb.astype(jnp.float32)
                im = imb.astype(jnp.float32)
                base = 4 * wide + s * 16
                rot_s[slot, base : base + 16, la] = reb
                rot_s[slot, base : base + 16, lb] = imb
                for k, (t1, t2, _, _) in enumerate(PAIRS):
                    co = tab_s[later, k : k + 1, la]
                    si = tab_s[later, 4 + k : 5 + k, la]
                    rc = re * co
                    is_ = im * si
                    ic = im * co
                    rs = re * si
                    b1 = t1 * wide + s * 16
                    b2 = t2 * wide + s * 16
                    rot_s[slot, b1 : b1 + 16, la] = (rc - is_).astype(jnp.bfloat16)
                    rot_s[slot, b1 : b1 + 16, lb] = (ic + rs).astype(jnp.bfloat16)
                    rot_s[slot, b2 : b2 + 16, la] = (rc + is_).astype(jnp.bfloat16)
                    rot_s[slot, b2 : b2 + 16, lb] = (ic - rs).astype(jnp.bfloat16)

    @pl.when(step == 0)
    def _():
        acc[...] = jnp.zeros_like(acc)
        rotate(0, 0, 0)

    def body(b, carry):
        acc[b] += lax.dot_general(
            rot_s[b % 2], part_s[...], NT_DIMS, preferred_element_type=jnp.float32
        )
        rotate(b + 1, (b + 1) % 2, jnp.where(b + 1 == pairs, 1, 0))
        return carry

    lax.fori_loop(0, pairs, body, 0)

    @pl.when(step == steps - 1)
    def _():
        my_y = ids[0]
        my_z = ids[1]
        my_c = ids[2]
        info = jnp.concatenate([m[...].astype(jnp.float32) for m in meta_y], axis=0)
        info = jnp.transpose(info).astype(jnp.int32)
        bins = info[8:9, :]
        r = lax.broadcasted_iota(jnp.int32, (META, np_), 0)
        spot = jnp.where((r % NBIN == bins) & (r < 3 * NBIN), -0.25, 0.0).astype(jnp.bfloat16)
        power_parts = jnp.concatenate([m[...] for m in meta_z], axis=0)
        power = jnp.dot(power_parts, spot, preferred_element_type=jnp.float32)
        for lt in range(np_ // 128):
            la = slice(lt * 128, lt * 128 + 128)
            for t in range(NT):
                sums = [jnp.zeros((piece, 128), jnp.float32) for _ in range(4)]
                for k in range(n_z):
                    z_abs = (my_z - offs_z[k] + n_z) % n_z
                    for u in range(2):
                        tile = (my_y * n_z + z_abs) * 2 + (my_c + u) % 2
                        lo = t * wide + (k % 2) * rows + u * piece
                        val = acc[k // 2, lo : lo + piece, la]
                        lo = k * rows + u * piece
                        val = val + power[lo : lo + piece, la]
                        for j in range(4):
                            sums[j] = jnp.where(info[j : j + 1, la] // 2 == tile, val, sums[j])
                for j in range(4):
                    x = sums[j]
                    start = info[4 + j : 5 + j, la]
                    for bit in (16, 8, 4, 2, 1):
                        x = jnp.where((start & bit) != 0, pltpu.roll(x, piece - bit, 0), x)
                    w_s[j, t * 16 : t * 16 + 16, la] = x[0:16]
        lane = lax.broadcasted_iota(jnp.int32, (1, np_), 1)
        k_of = lane // rows
        c_of = ((lane // piece) + my_c) % 2
        y_of = jnp.zeros((1, np_), jnp.int32)
        for k in range(n_y):
            y_of = jnp.where(k_of == k, (my_y - offs_y[k] + n_y) % n_y, y_of)
        per_row = 4 * n_z
        n_slots = out.shape[0]
        slot_row = lax.broadcasted_iota(jnp.int32, (n_slots, np_), 0)
        total = jnp.zeros(out.shape, jnp.float32)
        for j in range(4):
            local = info[j : j + 1, :] - my_y * per_row
            fits = (local >= 0) & (local < per_row)
            slot = jnp.where(fits, (y_of * 2 + c_of) * per_row + local, -1)
            pick = jnp.where(slot_row == slot, 1.0, 0.0).astype(jnp.bfloat16)
            for part in split3(w_s[j]):
                total = total + lax.dot_general(pick, part, NT_DIMS, preferred_element_type=jnp.float32)
        out[...] = total


def score(ids, y_pieces, z_pieces, tables):
    n_y = len(y_pieces) // 2
    n_z = len(z_pieces) // 2
    piece = y_pieces[0].shape[0]
    width = y_pieces[0].shape[1] - META
    span = 2 * CHUNK
    steps = width // span
    n_slots = 2 * n_y * 4 * n_z
    np_ = 2 * n_y * piece
    now = pl.BlockSpec((piece, span), lambda i, s: (0, i))
    later = pl.BlockSpec((piece, span), lambda i, s: (0, jnp.minimum(i + 1, steps - 1)))
    table = pl.BlockSpec((8, CHUNK), lambda i, s: (0, i))
    table_later = pl.BlockSpec((8, CHUNK), lambda i, s: (0, jnp.minimum(i + 1, steps - 1)))
    tail = pl.BlockSpec((piece, META), lambda i, s: (0, width // META))
    n_all = len(y_pieces) + len(z_pieces)
    flops = 2 * NT * (2 * n_z * piece) * np_ * width
    return pl.pallas_call(
        functools.partial(score_kernel, n_y, n_z),
        out_shape=jax.ShapeDtypeStruct((n_slots, NT * 16), jnp.float32),
        grid_spec=pltpu.PrefetchScalarGridSpec(
            num_scalar_prefetch=1,
            grid=(steps,),
            in_specs=[now] * n_all + [later] * 4 + [table, table_later] + [tail] * n_all,
            out_specs=pl.BlockSpec((n_slots, NT * 16), lambda i, s: (0, 0)),
            scratch_shapes=[
                pltpu.VMEM((np_, span), jnp.bfloat16),
                pltpu.VMEM((n_z // 2 + 1, 4 * piece, span), jnp.bfloat16),
                pltpu.VMEM((2, 8, CHUNK), jnp.float32),
                pltpu.VMEM((2, NT * 4 * piece, span), jnp.bfloat16),
                pltpu.VMEM((n_z // 2, NT * 4 * piece, np_), jnp.float32),
                pltpu.VMEM((4, NT * 16, np_), jnp.float32),
            ],
        ),
        compiler_params=pltpu.CompilerParams(
            dimension_semantics=("arbitrary",), vmem_limit_bytes=60 * 1024 * 1024
        ),
        cost_estimate=pl.CostEstimate(flops=flops, transcendentals=0, bytes_accessed=17 * 1024 * 1024),
        name="score",
    )(ids, *y_pieces, *z_pieces, *z_pieces[:4], tables, tables, *y_pieces, *z_pieces)


def all_rings(pieces, axes):
    n = lax.axis_size(axes[0])
    ahead = list(pieces)
    back = list(pieces)
    found = [[p] for p in pieces]

    def shift(v, axis, d):
        return lax.ppermute(v, axis, [(i, (i + d) % n) for i in range(n)])

    for s in range(1, n // 2 + 1):
        for k, axis in enumerate(axes):
            first = k < len(axes) // 2
            if s < n // 2:
                ahead[k] = shift(ahead[k], axis, 1)
                back[k] = shift(back[k], axis, -1)
                found[k] += [ahead[k], back[k]]
            elif first:
                found[k].append(shift(ahead[k], axis, 1))
            else:
                found[k].append(shift(back[k], axis, -1))
    return found


def slot_rank(tile_ids):
    positions = jnp.arange(tile_ids.shape[0], dtype=jnp.int32)
    earlier_same = (tile_ids[:, None] == tile_ids[None, :]) & (
        positions[None, :] < positions[:, None]
    )
    return jnp.sum(earlier_same.astype(jnp.int32), axis=1)


def finish(scored):
    row_peak = jnp.max(scored, axis=(1, 2))
    log_total = row_peak + jnp.log(jnp.sum(jnp.exp(scored - row_peak[:, None, None]), axis=(1, 2)))
    posterior = jnp.exp(scored - log_total[:, None, None])
    return (posterior, log_total)


def per_device(particles, projections, noise_weight, tile_list, ori_start, shifts, defocus_bin):
    band = lax.axis_index("shell")
    my_y = lax.axis_index(TILE[0])
    my_z = lax.axis_index(TILE[1])
    my_c = lax.axis_index(TILE[2])
    count, _, width = particles.shape
    windows = tile_list.shape[1]
    half = width // 2
    freq_x, freq_y = frequencies(band * width, width)
    ctf = ctf_table(freq_x, freq_y, NBIN)
    first_x = (band * width) // BOX
    span_x = first_x + jnp.arange(width // BOX, dtype=jnp.int32)
    span_y = jnp.arange(BOX, dtype=jnp.int32) - BOX // 2
    cx, sx = turn(span_x[None, :] * shifts[:, 0:1])
    cy, sy = turn(span_y[None, :] * shifts[:, 1:2])
    key = tile_list * 2 + slot_rank(tile_list.reshape(-1)).reshape(count, windows)
    meta = jnp.concatenate([key, ori_start, defocus_bin[:, None]], axis=1)
    meta = jnp.pad(meta, ((0, 0), (0, META - meta.shape[1]))).astype(jnp.bfloat16)
    y_keep, z_keep, send, energy = prepare(
        my_c.reshape(1).astype(jnp.int32),
        particles[:, 0],
        particles[:, 1],
        projections[:, 0],
        projections[:, 1],
        noise_weight[None, :],
        ctf,
        defocus_bin[:, None],
        cx,
        sx,
        cy,
        sy,
        meta,
    )
    got = lax.ppermute(send, TILE[2], [(0, 1), (1, 0)])
    found = all_rings([y_keep, z_keep, got[:count], got[count:]], [TILE[0], TILE[1], TILE[0], TILE[1]])
    y_pieces = [p for both in zip(found[0], found[2]) for p in both]
    z_pieces = [p for both in zip(found[1], found[3]) for p in both]
    mult = jnp.array([[a, b] for _, _, a, b in PAIRS], jnp.int32)
    fx = lax.dynamic_slice_in_dim(freq_x, my_c * half, half)
    fy = lax.dynamic_slice_in_dim(freq_y, my_c * half, half)
    co, si = turn(mult[:, 0:1] * fx[None, :] + mult[:, 1:2] * fy[None, :])
    tables = jnp.concatenate([co, si], axis=0)
    ids = jnp.stack([my_y, my_z, my_c]).astype(jnp.int32)
    slots = score(ids, y_pieces, z_pieces, tables)
    n_y = lax.axis_size(TILE[0])
    slots = slots.reshape(2 * n_y, -1, NT * 16)
    slots = lax.all_to_all(slots, (TILE[0], TILE[2]), split_axis=0, concat_axis=0, tiled=True)
    slots = jnp.sum(slots.reshape(n_y, 2, -1, NT * 16), axis=1).reshape(-1, NT * 16)
    items = jnp.take(slots, key.reshape(-1), axis=0)
    items = items.reshape(count, windows * NT * 16) - 0.5 * energy[:, 0:1]
    n_x = lax.axis_size("shell")
    copies = jnp.broadcast_to(items, (n_x, *items.shape))
    items = jnp.sum(lax.all_to_all(copies, "shell", split_axis=0, concat_axis=0, tiled=True), axis=0)
    scores = items.reshape(count, windows, NT, 16).transpose(0, 2, 1, 3).reshape(count, NT, windows * 16)
    return finish(scores)


def solution(mesh):
    split = Mesh(
        mesh.devices.reshape(8, 8, 2, mesh.shape["shell"]), ("tile_0", "tile_1", "tile_2", "shell")
    )
    in_specs = (
        P(TILE, None, "shell"),
        P(TILE, None, "shell"),
        P("shell"),
        P(TILE, None),
        P(TILE, None),
        P(TILE, None),
        P(TILE),
    )
    out_specs = (P(TILE, None, None), P(TILE))
    return jax.shard_map(
        per_device, mesh=split, in_specs=in_specs, out_specs=out_specs, check_vma=False
    )
```

```python
import functools
import math

import jax
import jax.numpy as jnp
from jax import lax
from jax.experimental import pallas as pl
from jax.experimental.pallas import tpu as pltpu
from jax.sharding import Mesh
from jax.sharding import PartitionSpec as P

BOX = 256
NBIN = 16
TSIDE = 3
NT = TSIDE * TSIDE
TILE = ("tile_0", "tile_1", "tile_2")

wave_length = 0.0197
aberration = 27000000.0
amplitude = 0.1
b_factor = 20.0
defocus_base = 5000.0
defocus_step = 500.0

META = 128
CHUNK = 1024
PAIRS = ((5, 3, 0, 1), (7, 1, 1, 0), (8, 0, 1, 1), (6, 2, 1, -1))


def ring_offsets(n):
    offs = [0]
    for s in range(1, n // 2):
        offs += [s, -s]
    return offs + [n // 2]


def frequencies(first_index, span_count):
    flat_index = first_index + jnp.arange(span_count, dtype=jnp.int32)
    freq_x = flat_index // BOX
    freq_y = flat_index % BOX - BOX // 2
    return (freq_x, freq_y)


def ctf_table(freq_x, freq_y, bins_count):
    scaled_x = freq_x.astype(jnp.float32) / BOX
    scaled_y = freq_y.astype(jnp.float32) / BOX
    radius_sq = scaled_x * scaled_x + scaled_y * scaled_y
    defocus = defocus_base + defocus_step * jnp.arange(bins_count, dtype=jnp.float32)[:, None]
    aberr_phase = (
        math.pi * wave_length * defocus * radius_sq[None, :]
        - 0.5 * math.pi * aberration * wave_length**3 * radius_sq[None, :] ** 2
    )
    envelope = jnp.exp(-0.25 * b_factor * radius_sq)[None, :]
    return (
        -(math.sqrt(1.0 - amplitude**2) * jnp.sin(aberr_phase) + amplitude * jnp.cos(aberr_phase))
        * envelope
    )


def turn(m):
    angles = jnp.mod(m, BOX).astype(jnp.float32) * (2.0 * math.pi / BOX)
    return (jnp.cos(angles), jnp.sin(angles))


def split3(v):
    hi = v.astype(jnp.bfloat16)
    rest = v - hi.astype(jnp.float32)
    mid = rest.astype(jnp.bfloat16)
    lo = (rest - mid.astype(jnp.float32)).astype(jnp.bfloat16)
    return hi, mid, lo


NT_DIMS = (((1,), (1,)), ((), ()))


def prep_kernel(c_ref, xr, xi, qr, qi, w, ctf, binc, cx, sx, cy, sy, meta, own_a, own_b, send, energy, wc2_s, mag_s):
    n, width = xr.shape
    half = width // 2
    c = c_ref[0]
    bins = binc[...]
    acc = jnp.zeros((n, BOX), jnp.float32)
    cyv = cy[...]
    syv = sy[...]

    first = c == 0

    def put(mine, place, own, other):
        for k in range(2):
            a = pl.ds(place + k * CHUNK, BOX)

            @pl.when(mine)
            def _(k=k, a=a):
                own_a[:, a] = own[k]
                send[n : 2 * n, a] = other[k]

            @pl.when(jnp.logical_not(mine))
            def _(k=k, a=a):
                own_b[:, a] = own[k]
                send[0:n, a] = other[k]

    for g in range(width // BOX):
        sl = pl.ds(g * BOX, BOX)
        wv = w[:, sl]
        table = ctf[:, sl]
        wc2_s[:, sl] = wv * table * table
        rows = jnp.zeros((n, BOX), jnp.float32)
        for b in range(NBIN):
            rows = jnp.where(bins == b, table[b : b + 1, :], rows)
        re = xr[:, sl].astype(jnp.float32)
        im = xi[:, sl].astype(jnp.float32)
        cxv = cx[:, g : g + 1]
        sxv = sx[:, g : g + 1]
        co = cxv * cyv - sxv * syv
        si = sxv * cyv + cxv * syv
        factor = wv * rows
        h = (g * BOX) // half
        at = g * BOX - h * half
        place = (at // CHUNK) * 2 * CHUNK + at % CHUNK
        wr = (factor * (re * co + im * si)).astype(jnp.bfloat16)
        wi = (factor * (im * co - re * si)).astype(jnp.bfloat16)
        acc = acc + wv * (re * re + im * im)
        pr = qr[:, sl]
        pi = qi[:, sl]
        own = (jnp.where(first, wr, pr), jnp.where(first, wi, pi))
        other = (jnp.where(first, pr, wr), jnp.where(first, pi, wi))
        put(c == h, place, own, other)
        prf = pr.astype(jnp.float32)
        pif = pi.astype(jnp.float32)
        mag_s[:, sl] = prf * prf + pif * pif
    energy[...] = jnp.broadcast_to(jnp.sum(acc, axis=1, keepdims=True), (n, META))
    power = lax.dot_general(
        mag_s[...], wc2_s[...], NT_DIMS, precision=lax.Precision.HIGHEST, preferred_element_type=jnp.float32
    )
    lane = lax.broadcasted_iota(jnp.int32, (NBIN, META), 1)
    row = lax.broadcasted_iota(jnp.int32, (NBIN, META), 0)
    placed = jnp.zeros((n, META), jnp.float32)
    for k, part in enumerate(split3(power)):
        spot = jnp.where(lane == row + k * NBIN, 1.0, 0.0).astype(jnp.bfloat16)
        placed = placed + jnp.dot(part, spot, preferred_element_type=jnp.float32)
    tail = pl.ds(width, META)
    placed = placed.astype(jnp.bfloat16)
    own = jnp.where(first, meta[...], placed)
    other = jnp.where(first, placed, meta[...])
    own_a[:, tail] = own
    own_b[:, tail] = own
    send[0:n, tail] = other
    send[n : 2 * n, tail] = other


def prepare(c, xr, xi, qr, qi, w, ctf, binc, cx, sx, cy, sy, meta):
    n, width = xr.shape
    vm = pl.BlockSpec(memory_space=pltpu.VMEM)
    return pl.pallas_call(
        prep_kernel,
        out_shape=(
            jax.ShapeDtypeStruct((n, width + META), jnp.bfloat16),
            jax.ShapeDtypeStruct((n, width + META), jnp.bfloat16),
            jax.ShapeDtypeStruct((2 * n, width + META), jnp.bfloat16),
            jax.ShapeDtypeStruct((n, META), jnp.float32),
        ),
        in_specs=[pl.BlockSpec(memory_space=pltpu.SMEM)] + [vm] * 12,
        out_specs=(vm, vm, vm, vm),
        scratch_shapes=[pltpu.VMEM((NBIN, width), jnp.float32), pltpu.VMEM((n, width), jnp.float32)],
        name="prep",
    )(c, xr, xi, qr, qi, w, ctf, binc, cx, sx, cy, sy, meta)


def score_kernel(n_pos, ids, *refs):
    it = iter(refs)
    take = lambda n: [next(it) for _ in range(n)]
    mine = take(n_pos + 1)
    theirs = take(n_pos + 1)
    mine_next = take(2)
    theirs_next = take(2)
    tables, tables_next = take(2)
    mine_meta = take(n_pos + 1)
    theirs_meta = take(n_pos + 1)
    out, part_s, proj_s, tab_s, rot_s, acc, w_s = take(7)
    step = pl.program_id(0)
    steps = pl.num_programs(0)
    rows = mine[0].shape[0]
    piece = rows // 2
    n_y = n_z = n_pos
    pairs = n_z // 2
    np_ = n_y * rows
    offs_y = ring_offsets(n_y)
    offs_z = ring_offsets(n_z)
    my_y = ids[0]
    my_z = ids[1]
    my_c = ids[2]

    def spread(y_refs, z_refs, z_later):
        at = 0
        for ref in y_refs:
            part_s[at : at + ref.shape[0], :] = ref[...]
            at += ref.shape[0]
        at = 0
        for ref in list(z_refs) + list(z_later):
            lo = at % (2 * rows)
            proj_s[at // (2 * rows), lo : lo + ref.shape[0], :] = ref[...]
            at += ref.shape[0]

    @pl.when(my_c == 0)
    def _():
        spread(mine, theirs, theirs_next)

    @pl.when(my_c != 0)
    def _():
        spread(theirs, mine, mine_next)

    tab_s[0] = tables[...]
    tab_s[1] = tables_next[...]

    def rotate(b, slot, later):
        for s in range(2 * rows // 16):
            sl = slice(s * 16, s * 16 + 16)
            i = s * 16 // rows
            at = s * 16 % rows
            for q in range(CHUNK // 256):
                la = slice(q * 256, q * 256 + 256)
                lb = slice(CHUNK + q * 256, CHUNK + q * 256 + 256)
                reb = proj_s[b, sl, la]
                imb = proj_s[b, sl, lb]
                re = reb.astype(jnp.float32)
                im = imb.astype(jnp.float32)
                base = 4 * rows + at
                rot_s[slot, i, base : base + 16, la] = reb
                rot_s[slot, i, base : base + 16, lb] = imb
                for k, (t1, t2, _, _) in enumerate(PAIRS):
                    co = tab_s[later, k : k + 1, la]
                    si = tab_s[later, 4 + k : 5 + k, la]
                    rc = re * co
                    is_ = im * si
                    ic = im * co
                    rs = re * si
                    b1 = t1 * rows + at
                    b2 = t2 * rows + at
                    rot_s[slot, i, b1 : b1 + 16, la] = (rc - is_).astype(jnp.bfloat16)
                    rot_s[slot, i, b1 : b1 + 16, lb] = (ic + rs).astype(jnp.bfloat16)
                    rot_s[slot, i, b2 : b2 + 16, la] = (rc + is_).astype(jnp.bfloat16)
                    rot_s[slot, i, b2 : b2 + 16, lb] = (ic - rs).astype(jnp.bfloat16)

    @pl.when(step == 0)
    def _():
        acc[...] = jnp.zeros_like(acc)
        rotate(0, 0, 0)

    def body(b, carry):
        for i in range(2):
            acc[2 * b + i] += lax.dot_general(
                rot_s[b % 2, i], part_s[...], NT_DIMS, preferred_element_type=jnp.float32
            )
        rotate(b + 1, (b + 1) % 2, jnp.where(b + 1 == pairs, 1, 0))
        return carry

    lax.fori_loop(0, pairs, body, 0)

    @pl.when(step == steps - 1)
    def _():
        a_meta = jnp.concatenate([m[...] for m in mine_meta], axis=0)
        b_meta = jnp.concatenate([m[...] for m in theirs_meta], axis=0)
        info = jnp.where(my_c == 0, a_meta, b_meta).astype(jnp.float32)
        power_parts = jnp.where(my_c == 0, b_meta, a_meta)
        info = jnp.transpose(info).astype(jnp.int32)
        bins = info[8:9, :]
        r = lax.broadcasted_iota(jnp.int32, (META, np_), 0)
        spot = jnp.where((r % NBIN == bins) & (r < 3 * NBIN), -0.25, 0.0).astype(jnp.bfloat16)
        power = jnp.dot(power_parts, spot, preferred_element_type=jnp.float32)
        for lt in range(np_ // 128):
            la = slice(lt * 128, lt * 128 + 128)
            for t in range(NT):
                sums = [jnp.zeros((piece, 128), jnp.float32) for _ in range(4)]
                for k in range(n_z):
                    z_abs = (my_z - offs_z[k] + n_z) % n_z
                    for u in range(2):
                        tile = (my_y * n_z + z_abs) * 2 + 1 - u
                        lo = t * rows + u * piece
                        val = acc[k, lo : lo + piece, la]
                        lo = k * rows + u * piece
                        val = val + power[lo : lo + piece, la]
                        for j in range(4):
                            sums[j] = jnp.where(info[j : j + 1, la] // 2 == tile, val, sums[j])
                for j in range(4):
                    x = sums[j]
                    start = info[4 + j : 5 + j, la]
                    for bit in (16, 8, 4, 2, 1):
                        x = jnp.where((start & bit) != 0, pltpu.roll(x, piece - bit, 0), x)
                    w_s[j, t * 16 : t * 16 + 16, la] = x[0:16]
        lane = lax.broadcasted_iota(jnp.int32, (1, np_), 1)
        k_of = lane // rows
        c_of = (lane // piece) % 2
        y_of = jnp.zeros((1, np_), jnp.int32)
        for k in range(n_y):
            y_of = jnp.where(k_of == k, (my_y - offs_y[k] + n_y) % n_y, y_of)
        per_row = 4 * n_z
        n_slots = out.shape[0]
        slot_row = lax.broadcasted_iota(jnp.int32, (n_slots, np_), 0)
        total = jnp.zeros(out.shape, jnp.float32)
        for j in range(4):
            local = info[j : j + 1, :] - my_y * per_row
            fits = (local >= 0) & (local < per_row)
            slot = jnp.where(fits, (y_of * 2 + c_of) * per_row + local, -1)
            pick = jnp.where(slot_row == slot, 1.0, 0.0).astype(jnp.bfloat16)
            for part in split3(w_s[j]):
                total = total + lax.dot_general(pick, part, NT_DIMS, preferred_element_type=jnp.float32)
        out[...] = total


def score(ids, mine, theirs, tables):
    n_pos = len(mine) - 1
    rows = mine[0].shape[0]
    width = mine[0].shape[1] - META
    span = 2 * CHUNK
    steps = width // span
    n_slots = 2 * n_pos * 4 * n_pos
    np_ = n_pos * rows
    after = lambda i, s: (0, jnp.minimum(i + 1, steps - 1))
    now = [pl.BlockSpec((a.shape[0], span), lambda i, s: (0, i)) for a in mine]
    later = pl.BlockSpec((rows, span), after)
    table = pl.BlockSpec((8, CHUNK), lambda i, s: (0, i))
    table_later = pl.BlockSpec((8, CHUNK), after)
    tail = [pl.BlockSpec((a.shape[0], META), lambda i, s: (0, width // META)) for a in mine]
    flops = 2 * NT * np_ * np_ * width
    return pl.pallas_call(
        functools.partial(score_kernel, n_pos),
        out_shape=jax.ShapeDtypeStruct((n_slots, NT * 16), jnp.float32),
        grid_spec=pltpu.PrefetchScalarGridSpec(
            num_scalar_prefetch=1,
            grid=(steps,),
            in_specs=now + now + [later] * 4 + [table, table_later] + tail + tail,
            out_specs=pl.BlockSpec((n_slots, NT * 16), lambda i, s: (0, 0)),
            scratch_shapes=[
                pltpu.VMEM((np_, span), jnp.bfloat16),
                pltpu.VMEM((n_pos // 2 + 1, 2 * rows, span), jnp.bfloat16),
                pltpu.VMEM((2, 8, CHUNK), jnp.float32),
                pltpu.VMEM((2, 2, NT * rows, span), jnp.bfloat16),
                pltpu.VMEM((n_pos, NT * rows, np_), jnp.float32),
                pltpu.VMEM((4, NT * 16, np_), jnp.float32),
            ],
        ),
        compiler_params=pltpu.CompilerParams(
            dimension_semantics=("arbitrary",), vmem_limit_bytes=60 * 1024 * 1024
        ),
        cost_estimate=pl.CostEstimate(flops=flops, transcendentals=0, bytes_accessed=17 * 1024 * 1024),
        name="score",
    )(ids, *mine, *theirs, *mine[:2], *theirs[:2], tables, tables, *mine, *theirs)


def core_rings(first, second, n):
    spot = lambda y, z, c: (y % n * n + z % n) * 2 + c
    cells = [(y, z) for y in range(n) for z in range(n)]

    def shift(v, d):
        pairs = [(spot(y, z, 0), spot(y + d, z, 0)) for y, z in cells]
        pairs += [(spot(y, z, 1), spot(y, z + d, 1)) for y, z in cells]
        return lax.ppermute(v, TILE, pairs)

    def swap(v):
        return lax.ppermute(v, TILE[2], [(0, 1), (1, 0)])

    ahead = [first, second]
    back = [first, second]
    theirs, mine = [swap(first)], [second]
    h = first.shape[0] // 2
    for s in range(1, n // 2 + 1):
        for k in range(2):
            if s < n // 2:
                ahead[k] = shift(ahead[k], 1)
                back[k] = shift(back[k], -1)
                new = [ahead[k], back[k]]
            else:
                new = [shift(ahead[k][:h], 1), shift(back[k][h:], -1)]
            if k == 0:
                theirs += [swap(v) for v in new]
            else:
                mine += new
    return mine, theirs


def slot_rank(tile_ids):
    positions = jnp.arange(tile_ids.shape[0], dtype=jnp.int32)
    earlier_same = (tile_ids[:, None] == tile_ids[None, :]) & (
        positions[None, :] < positions[:, None]
    )
    return jnp.sum(earlier_same.astype(jnp.int32), axis=1)


def finish(scored):
    row_peak = jnp.max(scored, axis=(1, 2))
    log_total = row_peak + jnp.log(jnp.sum(jnp.exp(scored - row_peak[:, None, None]), axis=(1, 2)))
    posterior = jnp.exp(scored - log_total[:, None, None])
    return (posterior, log_total)


def per_device(particles, projections, noise_weight, tile_list, ori_start, shifts, defocus_bin):
    band = lax.axis_index("shell")
    my_y = lax.axis_index(TILE[0])
    my_z = lax.axis_index(TILE[1])
    my_c = lax.axis_index(TILE[2])
    count, _, width = particles.shape
    windows = tile_list.shape[1]
    half = width // 2
    freq_x, freq_y = frequencies(band * width, width)
    ctf = ctf_table(freq_x, freq_y, NBIN)
    first_x = (band * width) // BOX
    span_x = first_x + jnp.arange(width // BOX, dtype=jnp.int32)
    span_y = jnp.arange(BOX, dtype=jnp.int32) - BOX // 2
    cx, sx = turn(span_x[None, :] * shifts[:, 0:1])
    cy, sy = turn(span_y[None, :] * shifts[:, 1:2])
    key = tile_list * 2 + slot_rank(tile_list.reshape(-1)).reshape(count, windows)
    meta = jnp.concatenate([key, ori_start, defocus_bin[:, None]], axis=1)
    meta = jnp.pad(meta, ((0, 0), (0, META - meta.shape[1]))).astype(jnp.bfloat16)
    own_a, own_b, send, energy = prepare(
        my_c.reshape(1).astype(jnp.int32),
        particles[:, 0],
        particles[:, 1],
        projections[:, 0],
        projections[:, 1],
        noise_weight[None, :],
        ctf,
        defocus_bin[:, None],
        cx,
        sx,
        cy,
        sy,
        meta,
    )
    got = lax.ppermute(send, TILE[2], [(0, 1), (1, 0)])
    kept = jnp.concatenate([own_a, got[:count]], axis=0)
    passed = jnp.concatenate([own_b, got[count:]], axis=0)
    mine, theirs = core_rings(passed, kept, lax.axis_size(TILE[0]))
    mult = jnp.array([[a, b] for _, _, a, b in PAIRS], jnp.int32)
    fx = lax.dynamic_slice_in_dim(freq_x, my_c * half, half)
    fy = lax.dynamic_slice_in_dim(freq_y, my_c * half, half)
    co, si = turn(mult[:, 0:1] * fx[None, :] + mult[:, 1:2] * fy[None, :])
    tables = jnp.concatenate([co, si], axis=0)
    ids = jnp.stack([my_y, my_z, my_c]).astype(jnp.int32)
    slots = score(ids, mine, theirs, tables)
    n_y = lax.axis_size(TILE[0])
    slots = slots.reshape(2 * n_y, -1, NT * 16)
    slots = lax.all_to_all(slots, (TILE[0], TILE[2]), split_axis=0, concat_axis=0, tiled=True)
    slots = jnp.sum(slots.reshape(n_y, 2, -1, NT * 16), axis=1).reshape(-1, NT * 16)
    items = jnp.take(slots, key.reshape(-1), axis=0)
    items = items.reshape(count, windows * NT * 16) - 0.5 * energy[:, 0:1]
    n_x = lax.axis_size("shell")
    copies = jnp.broadcast_to(items, (n_x, *items.shape))
    items = jnp.sum(lax.all_to_all(copies, "shell", split_axis=0, concat_axis=0, tiled=True), axis=0)
    scores = items.reshape(count, windows, NT, 16).transpose(0, 2, 1, 3).reshape(count, NT, windows * 16)
    return finish(scores)


def solution(mesh):
    split = Mesh(
        mesh.devices.reshape(8, 8, 2, mesh.shape["shell"]), ("tile_0", "tile_1", "tile_2", "shell")
    )
    in_specs = (
        P(TILE, None, "shell"),
        P(TILE, None, "shell"),
        P("shell"),
        P(TILE, None),
        P(TILE, None),
        P(TILE, None),
        P(TILE),
    )
    out_specs = (P(TILE, None, None), P(TILE))
    return jax.shard_map(
        per_device, mesh=split, in_specs=in_specs, out_specs=out_specs, check_vma=False
    )
```

```python
import functools
import math

import jax
import jax.numpy as jnp
from jax import lax
from jax.experimental import pallas as pl
from jax.experimental.pallas import tpu as pltpu
from jax.sharding import Mesh
from jax.sharding import PartitionSpec as P

BOX = 256
NBIN = 16
TSIDE = 3
NT = TSIDE * TSIDE
TILE = ("tile_0", "tile_1", "tile_2")

wave_length = 0.0197
aberration = 27000000.0
amplitude = 0.1
b_factor = 20.0
defocus_base = 5000.0
defocus_step = 500.0

META = 128
TURN = 2
CHUNK = 1024
PAIRS = ((5, 3, 0, 1), (7, 1, 1, 0), (8, 0, 1, 1), (6, 2, 1, -1))


def ring_offsets(n):
    offs = [0]
    for s in range(1, n // 2):
        offs += [s, -s]
    return offs + [n // 2]


def frequencies(first_index, span_count):
    flat_index = first_index + jnp.arange(span_count, dtype=jnp.int32)
    freq_x = flat_index // BOX
    freq_y = flat_index % BOX - BOX // 2
    return (freq_x, freq_y)


def ctf_table(freq_x, freq_y, bins_count):
    scaled_x = freq_x.astype(jnp.float32) / BOX
    scaled_y = freq_y.astype(jnp.float32) / BOX
    radius_sq = scaled_x * scaled_x + scaled_y * scaled_y
    defocus = defocus_base + defocus_step * jnp.arange(bins_count, dtype=jnp.float32)[:, None]
    aberr_phase = (
        math.pi * wave_length * defocus * radius_sq[None, :]
        - 0.5 * math.pi * aberration * wave_length**3 * radius_sq[None, :] ** 2
    )
    envelope = jnp.exp(-0.25 * b_factor * radius_sq)[None, :]
    return (
        -(math.sqrt(1.0 - amplitude**2) * jnp.sin(aberr_phase) + amplitude * jnp.cos(aberr_phase))
        * envelope
    )


def turn(m):
    angles = jnp.mod(m, BOX).astype(jnp.float32) * (2.0 * math.pi / BOX)
    return (jnp.cos(angles), jnp.sin(angles))


def split3(v):
    hi = v.astype(jnp.bfloat16)
    rest = v - hi.astype(jnp.float32)
    mid = rest.astype(jnp.bfloat16)
    lo = (rest - mid.astype(jnp.float32)).astype(jnp.bfloat16)
    return hi, mid, lo


NT_DIMS = (((1,), (1,)), ((), ()))


def prep_kernel(
    c_ref, x, q, w, ctf, binc, cx, sx, cy, sy, meta, own_a, own_b, send, energy, wc2_s, mag_s, x_s, q_s
):
    n = x.shape[0] // 2
    width = x.shape[1]
    real = pl.ds(0, n, stride=2)
    imag = pl.ds(1, n, stride=2)
    half = width // 2
    c = c_ref[0]
    bins = binc[...]
    acc = jnp.zeros((n, BOX), jnp.float32)
    cyv = cy[...]
    syv = sy[...]

    first = c == 0

    def put(mine, place, own, other):
        for k in range(2):
            a = pl.ds(place + k * CHUNK, BOX)

            @pl.when(mine)
            def _(k=k, a=a):
                own_a[:, a] = own[k]
                send[n : 2 * n, a] = other[k]

            @pl.when(jnp.logical_not(mine))
            def _(k=k, a=a):
                own_b[:, a] = own[k]
                send[0:n, a] = other[k]

    for g in range(width // BOX):
        sl = pl.ds(g * BOX, BOX)
        wv = w[:, sl]
        table = ctf[:, sl]
        wc2_s[:, sl] = wv * table * table
        rows = jnp.zeros((n, BOX), jnp.float32)
        for b in range(NBIN):
            rows = jnp.where(bins == b, table[b : b + 1, :], rows)
        x_s[g % 2, 0] = x[:, pl.ds(g * BOX, BOX // 2)].astype(jnp.float32)
        x_s[g % 2, 1] = x[:, pl.ds(g * BOX + BOX // 2, BOX // 2)].astype(jnp.float32)
        q_s[g % 2, 0] = q[:, pl.ds(g * BOX, BOX // 2)].astype(jnp.float32)
        q_s[g % 2, 1] = q[:, pl.ds(g * BOX + BOX // 2, BOX // 2)].astype(jnp.float32)
        whole = lambda ref, part: jnp.concatenate([ref[g % 2, i, part, :] for i in range(2)], axis=1)
        re = whole(x_s, real)
        im = whole(x_s, imag)
        cxv = cx[:, g : g + 1]
        sxv = sx[:, g : g + 1]
        co = cxv * cyv - sxv * syv
        si = sxv * cyv + cxv * syv
        factor = wv * rows
        h = (g * BOX) // half
        at = g * BOX - h * half
        place = (at // CHUNK) * 2 * CHUNK + at % CHUNK
        wr = (factor * (re * co + im * si)).astype(jnp.bfloat16)
        wi = (factor * (im * co - re * si)).astype(jnp.bfloat16)
        acc = acc + wv * (re * re + im * im)
        prf = whole(q_s, real)
        pif = whole(q_s, imag)
        pr = prf.astype(jnp.bfloat16)
        pi = pif.astype(jnp.bfloat16)
        own = (jnp.where(first, wr, pr), jnp.where(first, wi, pi))
        other = (jnp.where(first, pr, wr), jnp.where(first, pi, wi))
        put(c == h, place, own, other)
        mag_s[:, sl] = prf * prf + pif * pif
    energy[...] = jnp.broadcast_to(jnp.sum(acc, axis=1, keepdims=True), (n, META))
    power = lax.dot_general(
        mag_s[...], wc2_s[...], NT_DIMS, precision=lax.Precision.HIGHEST, preferred_element_type=jnp.float32
    )
    lane = lax.broadcasted_iota(jnp.int32, (NBIN, META), 1)
    row = lax.broadcasted_iota(jnp.int32, (NBIN, META), 0)
    placed = jnp.zeros((n, META), jnp.float32)
    for k, part in enumerate(split3(power)):
        spot = jnp.where(lane == row + k * NBIN, 1.0, 0.0).astype(jnp.bfloat16)
        placed = placed + jnp.dot(part, spot, preferred_element_type=jnp.float32)
    tail = pl.ds(width, META)
    placed = placed.astype(jnp.bfloat16)
    own = jnp.where(first, meta[...], placed)
    other = jnp.where(first, placed, meta[...])
    own_a[:, tail] = own
    own_b[:, tail] = own
    send[0:n, tail] = other
    send[n : 2 * n, tail] = other


def prepare(c, x, q, w, ctf, binc, cx, sx, cy, sy, meta):
    n = x.shape[0] // 2
    width = x.shape[1]
    vm = pl.BlockSpec(memory_space=pltpu.VMEM)
    return pl.pallas_call(
        prep_kernel,
        out_shape=(
            jax.ShapeDtypeStruct((n, width + META), jnp.bfloat16),
            jax.ShapeDtypeStruct((n, width + META), jnp.bfloat16),
            jax.ShapeDtypeStruct((2 * n, width + META), jnp.bfloat16),
            jax.ShapeDtypeStruct((n, META), jnp.float32),
        ),
        in_specs=[pl.BlockSpec(memory_space=pltpu.SMEM)] + [vm] * 10,
        out_specs=(vm, vm, vm, vm),
        scratch_shapes=[
            pltpu.VMEM((NBIN, width), jnp.float32),
            pltpu.VMEM((n, width), jnp.float32),
            pltpu.VMEM((2, 2, 2 * n, BOX // 2), jnp.float32),
            pltpu.VMEM((2, 2, 2 * n, BOX // 2), jnp.float32),
        ],
        name="prep",
    )(c, x, q, w, ctf, binc, cx, sx, cy, sy, meta)


def score_kernel(n_pos, ids, *refs):
    it = iter(refs)
    take = lambda n: [next(it) for _ in range(n)]
    mine = take(n_pos + 1)
    theirs = take(n_pos + 1)
    mine_next = take(2)
    theirs_next = take(2)
    tables, tables_next = take(2)
    mine_meta = take(n_pos + 1)
    theirs_meta = take(n_pos + 1)
    out, part_s, proj_s, tab_s, rot_s, acc, w_s, pick_s, slot_s, label_s = take(10)
    step = pl.program_id(0)
    steps = pl.num_programs(0)
    rows = mine[0].shape[0]
    piece = rows // 2
    n_y = n_z = n_pos
    turns = 2 * n_z // TURN
    np_ = n_y * rows
    offs_y = ring_offsets(n_y)
    offs_z = ring_offsets(n_z)
    my_y = ids[0]
    my_z = ids[1]
    my_c = ids[2]

    def spread(y_refs, z_refs, z_later):
        at = 0
        for ref in y_refs:
            part_s[at : at + ref.shape[0], :] = ref[...]
            at += ref.shape[0]
        at = 0
        for ref in list(z_refs) + list(z_later):
            for i in range(ref.shape[0] // piece):
                tile = at // piece + i
                lo = tile % TURN * piece
                if tile // TURN <= turns:
                    proj_s[tile // TURN, lo : lo + piece, :] = ref[i * piece : (i + 1) * piece, :]
            at += ref.shape[0]

    @pl.when(my_c == 0)
    def _():
        spread(mine, theirs, theirs_next)

    @pl.when(my_c != 0)
    def _():
        spread(theirs, mine, mine_next)

    tab_s[0] = tables[...]
    tab_s[1] = tables_next[...]

    def rotate(b, slot, later):
        for s in range(TURN * piece // 16):
            sl = slice(s * 16, s * 16 + 16)
            i = s * 16 // piece
            at = s * 16 % piece
            for q in range(CHUNK // 256):
                la = slice(q * 256, q * 256 + 256)
                lb = slice(CHUNK + q * 256, CHUNK + q * 256 + 256)
                reb = proj_s[b, sl, la]
                imb = proj_s[b, sl, lb]
                re = reb.astype(jnp.float32)
                im = imb.astype(jnp.float32)
                base = (i * NT + 4) * piece + at
                rot_s[slot, base : base + 16, la] = reb
                rot_s[slot, base : base + 16, lb] = imb
                for k, (t1, t2, _, _) in enumerate(PAIRS):
                    co = tab_s[later, k : k + 1, la]
                    si = tab_s[later, 4 + k : 5 + k, la]
                    rc = re * co
                    is_ = im * si
                    ic = im * co
                    rs = re * si
                    b1 = (i * NT + t1) * piece + at
                    b2 = (i * NT + t2) * piece + at
                    rot_s[slot, b1 : b1 + 16, la] = (rc - is_).astype(jnp.bfloat16)
                    rot_s[slot, b1 : b1 + 16, lb] = (ic + rs).astype(jnp.bfloat16)
                    rot_s[slot, b2 : b2 + 16, la] = (rc + is_).astype(jnp.bfloat16)
                    rot_s[slot, b2 : b2 + 16, lb] = (ic - rs).astype(jnp.bfloat16)

    def window_slots(info):
        lane = lax.broadcasted_iota(jnp.int32, (1, np_), 1)
        slots = []
        for j in range(4):
            key = info[j : j + 1, :]
            local = key // 2 - my_y * 2 * n_z
            k_of = jnp.full((1, np_), -1, jnp.int32)
            for k in range(n_z):
                z_abs = (my_z - offs_z[k] + n_z) % n_z
                k_of = jnp.where((local >= 0) & (local // 2 == z_abs), k, k_of)
            slot = k_of * rows + (1 - local % 2) * piece + (lane // piece) * 2 + key % 2
            slots.append(jnp.where(k_of >= 0, slot, -1))
        return slots

    @pl.when(step == 0)
    def _():
        acc[...] = jnp.zeros_like(acc)
        rotate(0, 0, 0)
        a_meta = jnp.concatenate([m[...] for m in mine_meta], axis=0)
        b_meta = jnp.concatenate([m[...] for m in theirs_meta], axis=0)
        info_f = jnp.transpose(jnp.where(my_c == 0, a_meta, b_meta).astype(jnp.float32))
        info = info_f.astype(jnp.int32)
        slot_row = lax.broadcasted_iota(jnp.int32, (np_, np_), 0)
        which = lax.broadcasted_iota(jnp.int32, (8, np_), 0)
        total = jnp.zeros((np_, np_), jnp.float32)
        labels = jnp.zeros((8, np_), jnp.float32)
        for j, slot in enumerate(window_slots(info)):
            hit = jnp.where(slot_row == slot, 1.0, 0.0)
            total = total + hit
            values = jnp.where(which == 0, info_f[4 + j : 5 + j, :], info_f[8:9, :])
            labels = labels + lax.dot_general(
                values.astype(jnp.bfloat16),
                hit.astype(jnp.bfloat16),
                NT_DIMS,
                preferred_element_type=jnp.float32,
            )
        pick_s[...] = total.astype(jnp.bfloat16)
        label_s[...] = labels.astype(jnp.int32)

    for g in range(2):
        for q in range(4):
            la = slice(q * CHUNK // 2, (q + 1) * CHUNK // 2)
            slot_s[g, :, la] = jnp.dot(
                pick_s[g * np_ // 2 : (g + 1) * np_ // 2, :], part_s[:, la], preferred_element_type=jnp.float32
            ).astype(jnp.bfloat16)

    def body(b, carry):
        rotate(b + 1, (b + 1) % 2, jnp.where(b + 1 == turns, 1, 0))
        scored = lax.dot_general(
            rot_s[b % 2], slot_s[b // (turns // 2)], NT_DIMS, preferred_element_type=jnp.float32
        )
        for i in range(TURN):
            acc[b * TURN + i] += scored[i * NT * piece : (i + 1) * NT * piece]
        return carry

    lax.fori_loop(0, turns, body, 0)

    @pl.when(step == steps - 1)
    def _():
        a_meta = jnp.concatenate([m[...] for m in mine_meta], axis=0)
        b_meta = jnp.concatenate([m[...] for m in theirs_meta], axis=0)
        power_parts = jnp.where(my_c == 0, b_meta, a_meta)
        starts = label_s[0:1, :]
        bins = label_s[1:2, :]
        r = lax.broadcasted_iota(jnp.int32, (META, np_), 0)
        spot = jnp.where((r % NBIN == bins) & (r < 3 * NBIN), -0.25, 0.0).astype(jnp.bfloat16)
        power = jnp.dot(power_parts, spot, preferred_element_type=jnp.float32)
        section = lax.broadcasted_iota(jnp.int32, (1, 128), 1) // piece
        for lt in range(np_ // 128):
            la = slice(lt * 128, lt * 128 + 128)
            lo = lt % 2 * 128
            start = starts[:, la]
            tiles = [(2 * lt + i // 2, i % 2) for i in range(4)]
            level = jnp.zeros((piece, 128), jnp.float32)
            for i, (k, u) in enumerate(tiles):
                first = k * rows + u * piece
                level = jnp.where(section == i, power[first : first + piece, la], level)
            for t in range(NT):
                x = jnp.zeros((piece, 128), jnp.float32)
                for i, (k, u) in enumerate(tiles):
                    first = t * piece
                    x = jnp.where(section == i, acc[2 * k + u, first : first + piece, lo : lo + 128], x)
                x = x + level
                for bit in (16, 8, 4, 2, 1):
                    x = jnp.where((start & bit) != 0, pltpu.roll(x, piece - bit, 0), x)
                w_s[t * 16 : t * 16 + 16, la] = x[0:16]
        lane = lax.broadcasted_iota(jnp.int32, (1, np_), 1)
        z_of = jnp.zeros((1, np_), jnp.int32)
        y_of = jnp.zeros((1, np_), jnp.int32)
        block = lane % piece // 2
        for k in range(n_pos):
            z_of = jnp.where(lane // rows == k, (my_z - offs_z[k] + n_z) % n_z, z_of)
            y_of = jnp.where(block // 2 == k, (my_y - offs_y[k] + n_y) % n_y, y_of)
        tile = z_of * 2 + 1 - lane // piece % 2
        place = (y_of * 2 + block % 2) * 4 * n_z + tile * 2 + lane % 2
        slot_row = lax.broadcasted_iota(jnp.int32, (out.shape[0], np_), 0)
        moved = jnp.where(slot_row == place, 1.0, 0.0).astype(jnp.bfloat16)
        total = jnp.zeros(out.shape, jnp.float32)
        for part in split3(w_s[...]):
            total = total + lax.dot_general(moved, part, NT_DIMS, preferred_element_type=jnp.float32)
        out[...] = total


def score(ids, mine, theirs, tables):
    n_pos = len(mine) - 1
    rows = mine[0].shape[0]
    piece = rows // 2
    width = mine[0].shape[1] - META
    span = 2 * CHUNK
    steps = width // span
    n_slots = 2 * n_pos * 4 * n_pos
    np_ = n_pos * rows
    after = lambda i, s: (0, jnp.minimum(i + 1, steps - 1))
    now = [pl.BlockSpec((a.shape[0], span), lambda i, s: (0, i)) for a in mine]
    later = pl.BlockSpec((rows, span), after)
    table = pl.BlockSpec((8, CHUNK), lambda i, s: (0, i))
    table_later = pl.BlockSpec((8, CHUNK), after)
    tail = [pl.BlockSpec((a.shape[0], META), lambda i, s: (0, width // META)) for a in mine]
    flops = (NT + 1) * np_ * np_ * width
    return pl.pallas_call(
        functools.partial(score_kernel, n_pos),
        out_shape=jax.ShapeDtypeStruct((n_slots, NT * 16), jnp.float32),
        grid_spec=pltpu.PrefetchScalarGridSpec(
            num_scalar_prefetch=1,
            grid=(steps,),
            in_specs=now + now + [later] * 4 + [table, table_later] + tail + tail,
            out_specs=pl.BlockSpec((n_slots, NT * 16), lambda i, s: (0, 0)),
            scratch_shapes=[
                pltpu.VMEM((np_, span), jnp.bfloat16),
                pltpu.VMEM((2 * n_pos // TURN + 1, TURN * piece, span), jnp.bfloat16),
                pltpu.VMEM((2, 8, CHUNK), jnp.float32),
                pltpu.VMEM((2, NT * TURN * piece, span), jnp.bfloat16),
                pltpu.VMEM((2 * n_pos, NT * piece, np_ // 2), jnp.float32),
                pltpu.VMEM((NT * 16, np_), jnp.float32),
                pltpu.VMEM((np_, np_), jnp.bfloat16),
                pltpu.VMEM((2, np_ // 2, span), jnp.bfloat16),
                pltpu.VMEM((8, np_), jnp.int32),
            ],
        ),
        compiler_params=pltpu.CompilerParams(
            dimension_semantics=("arbitrary",),
            vmem_limit_bytes=60 * 1024 * 1024,
        ),
        cost_estimate=pl.CostEstimate(flops=flops, transcendentals=0, bytes_accessed=17 * 1024 * 1024),
        name="score",
    )(ids, *mine, *theirs, *mine[:2], *theirs[:2], tables, tables, *mine, *theirs)


def core_rings(first, second, n):
    spot = lambda y, z, c: (y % n * n + z % n) * 2 + c
    cells = [(y, z) for y in range(n) for z in range(n)]

    def shift(v, d):
        pairs = [(spot(y, z, 0), spot(y + d, z, 0)) for y, z in cells]
        pairs += [(spot(y, z, 1), spot(y, z + d, 1)) for y, z in cells]
        return lax.ppermute(v, TILE, pairs)

    def swap(v):
        return lax.ppermute(v, TILE[2], [(0, 1), (1, 0)])

    ahead = [first, second]
    back = [first, second]
    theirs, mine = [swap(first)], [second]
    h = first.shape[0] // 2
    for s in range(1, n // 2 + 1):
        for k in range(2):
            if s < n // 2:
                ahead[k] = shift(ahead[k], 1)
                back[k] = shift(back[k], -1)
                new = [ahead[k], back[k]]
            else:
                new = [shift(ahead[k][:h], 1), shift(back[k][h:], -1)]
            if k == 0:
                theirs += [swap(v) for v in new]
            else:
                mine += new
    return mine, theirs


def slot_rank(tile_ids):
    positions = jnp.arange(tile_ids.shape[0], dtype=jnp.int32)
    earlier_same = (tile_ids[:, None] == tile_ids[None, :]) & (
        positions[None, :] < positions[:, None]
    )
    return jnp.sum(earlier_same.astype(jnp.int32), axis=1)


def finish(scored):
    row_peak = jnp.max(scored, axis=(1, 2))
    log_total = row_peak + jnp.log(jnp.sum(jnp.exp(scored - row_peak[:, None, None]), axis=(1, 2)))
    posterior = jnp.exp(scored - log_total[:, None, None])
    return (posterior, log_total)


def per_device(particles, projections, noise_weight, tile_list, ori_start, shifts, defocus_bin):
    band = lax.axis_index("shell")
    my_y = lax.axis_index(TILE[0])
    my_z = lax.axis_index(TILE[1])
    my_c = lax.axis_index(TILE[2])
    count, _, width = particles.shape
    windows = tile_list.shape[1]
    half = width // 2
    freq_x, freq_y = frequencies(band * width, width)
    ctf = ctf_table(freq_x, freq_y, NBIN)
    first_x = (band * width) // BOX
    span_x = first_x + jnp.arange(width // BOX, dtype=jnp.int32)
    span_y = jnp.arange(BOX, dtype=jnp.int32) - BOX // 2
    cx, sx = turn(span_x[None, :] * shifts[:, 0:1])
    cy, sy = turn(span_y[None, :] * shifts[:, 1:2])
    key = tile_list * 2 + slot_rank(tile_list.reshape(-1)).reshape(count, windows)
    meta = jnp.concatenate([key, ori_start, defocus_bin[:, None]], axis=1)
    meta = jnp.pad(meta, ((0, 0), (0, META - meta.shape[1]))).astype(jnp.bfloat16)
    own_a, own_b, send, energy = prepare(
        my_c.reshape(1).astype(jnp.int32),
        particles.reshape(2 * count, width),
        projections.reshape(2 * count, width),
        noise_weight[None, :],
        ctf,
        defocus_bin[:, None],
        cx,
        sx,
        cy,
        sy,
        meta,
    )
    got = lax.ppermute(send, TILE[2], [(0, 1), (1, 0)])
    kept = jnp.concatenate([own_a, got[:count]], axis=0)
    passed = jnp.concatenate([own_b, got[count:]], axis=0)
    mine, theirs = core_rings(passed, kept, lax.axis_size(TILE[0]))
    mult = jnp.array([[a, b] for _, _, a, b in PAIRS], jnp.int32)
    fx = lax.dynamic_slice_in_dim(freq_x, my_c * half, half)
    fy = lax.dynamic_slice_in_dim(freq_y, my_c * half, half)
    co, si = turn(mult[:, 0:1] * fx[None, :] + mult[:, 1:2] * fy[None, :])
    tables = jnp.concatenate([co, si], axis=0)
    ids = jnp.stack([my_y, my_z, my_c]).astype(jnp.int32)
    slots = score(ids, mine, theirs, tables)
    n_y = lax.axis_size(TILE[0])
    slots = slots.reshape(2 * n_y, -1, NT * 16)
    slots = lax.all_to_all(slots, (TILE[0], TILE[2]), split_axis=0, concat_axis=0, tiled=True)
    slots = jnp.sum(slots.reshape(n_y, 2, -1, NT * 16), axis=1).reshape(-1, NT * 16)
    items = jnp.take(slots, key.reshape(-1), axis=0)
    items = items.reshape(count, windows * NT * 16) - 0.5 * energy[:, 0:1]
    n_x = lax.axis_size("shell")
    copies = jnp.broadcast_to(items, (n_x, *items.shape))
    items = jnp.sum(lax.all_to_all(copies, "shell", split_axis=0, concat_axis=0, tiled=True), axis=0)
    scores = items.reshape(count, windows, NT, 16).transpose(0, 2, 1, 3).reshape(count, NT, windows * 16)
    return finish(scores)


def solution(mesh):
    split = Mesh(
        mesh.devices.reshape(8, 8, 2, mesh.shape["shell"]), ("tile_0", "tile_1", "tile_2", "shell")
    )
    in_specs = (
        P(TILE, None, "shell"),
        P(TILE, None, "shell"),
        P("shell"),
        P(TILE, None),
        P(TILE, None),
        P(TILE, None),
        P(TILE),
    )
    out_specs = (P(TILE, None, None), P(TILE))
    return jax.shard_map(
        per_device, mesh=split, in_specs=in_specs, out_specs=out_specs, check_vma=False
    )
```

```python
import functools
import math

import jax
import jax.numpy as jnp
from jax import lax
from jax.experimental import pallas as pl
from jax.experimental.pallas import tpu as pltpu
from jax.sharding import Mesh
from jax.sharding import PartitionSpec as P

BOX = 256
NBIN = 16
TSIDE = 3
NT = TSIDE * TSIDE
TILE = ("tile_0", "tile_1", "tile_2")

wave_length = 0.0197
aberration = 27000000.0
amplitude = 0.1
b_factor = 20.0
defocus_base = 5000.0
defocus_step = 500.0

META = 128
TURN = 2
CHUNK = 1024
PAIRS = ((5, 3, 0, 1), (7, 1, 1, 0), (8, 0, 1, 1), (6, 2, 1, -1))


def ring_offsets(n):
    offs = [0]
    for s in range(1, n // 2):
        offs += [s, -s]
    return offs + [n // 2]


def frequencies(first_index, span_count):
    flat_index = first_index + jnp.arange(span_count, dtype=jnp.int32)
    freq_x = flat_index // BOX
    freq_y = flat_index % BOX - BOX // 2
    return (freq_x, freq_y)


def ctf_table(freq_x, freq_y, bins_count):
    scaled_x = freq_x.astype(jnp.float32) / BOX
    scaled_y = freq_y.astype(jnp.float32) / BOX
    radius_sq = scaled_x * scaled_x + scaled_y * scaled_y
    defocus = defocus_base + defocus_step * jnp.arange(bins_count, dtype=jnp.float32)[:, None]
    aberr_phase = (
        math.pi * wave_length * defocus * radius_sq[None, :]
        - 0.5 * math.pi * aberration * wave_length**3 * radius_sq[None, :] ** 2
    )
    envelope = jnp.exp(-0.25 * b_factor * radius_sq)[None, :]
    return (
        -(math.sqrt(1.0 - amplitude**2) * jnp.sin(aberr_phase) + amplitude * jnp.cos(aberr_phase))
        * envelope
    )


def turn(m):
    angles = jnp.mod(m, BOX).astype(jnp.float32) * (2.0 * math.pi / BOX)
    return (jnp.cos(angles), jnp.sin(angles))


def split3(v):
    hi = v.astype(jnp.bfloat16)
    rest = v - hi.astype(jnp.float32)
    mid = rest.astype(jnp.bfloat16)
    lo = (rest - mid.astype(jnp.float32)).astype(jnp.bfloat16)
    return hi, mid, lo


NT_DIMS = (((1,), (1,)), ((), ()))


def prep_kernel(
    c_ref, x, q, w, ctf, binc, cx, sx, cy, sy, meta, own_a, own_b, send, energy, wc2_s, mag_s, x_s, q_s
):
    n = x.shape[0] // 2
    width = x.shape[1]
    real = pl.ds(0, n, stride=2)
    imag = pl.ds(1, n, stride=2)
    half = width // 2
    c = c_ref[0]
    bins = binc[...]
    acc = jnp.zeros((n, BOX), jnp.float32)
    cyv = cy[...]
    syv = sy[...]

    first = c == 0

    def put(mine, place, own, other):
        for k in range(2):
            a = pl.ds(place + k * CHUNK, BOX)

            @pl.when(mine)
            def _(k=k, a=a):
                own_a[:, a] = own[k]
                send[n : 2 * n, a] = other[k]

            @pl.when(jnp.logical_not(mine))
            def _(k=k, a=a):
                own_b[:, a] = own[k]
                send[0:n, a] = other[k]

    for g in range(width // BOX):
        sl = pl.ds(g * BOX, BOX)
        wv = w[:, sl]
        table = ctf[:, sl]
        wc2_s[:, sl] = wv * table * table
        rows = jnp.zeros((n, BOX), jnp.float32)
        for b in range(NBIN):
            rows = jnp.where(bins == b, table[b : b + 1, :], rows)
        x_s[g % 2, 0] = x[:, pl.ds(g * BOX, BOX // 2)].astype(jnp.float32)
        x_s[g % 2, 1] = x[:, pl.ds(g * BOX + BOX // 2, BOX // 2)].astype(jnp.float32)
        q_s[g % 2, 0] = q[:, pl.ds(g * BOX, BOX // 2)].astype(jnp.float32)
        q_s[g % 2, 1] = q[:, pl.ds(g * BOX + BOX // 2, BOX // 2)].astype(jnp.float32)
        whole = lambda ref, part: jnp.concatenate([ref[g % 2, i, part, :] for i in range(2)], axis=1)
        re = whole(x_s, real)
        im = whole(x_s, imag)
        cxv = cx[:, g : g + 1]
        sxv = sx[:, g : g + 1]
        co = cxv * cyv - sxv * syv
        si = sxv * cyv + cxv * syv
        factor = wv * rows
        h = (g * BOX) // half
        at = g * BOX - h * half
        place = (at // CHUNK) * 2 * CHUNK + at % CHUNK
        wr = (factor * (re * co + im * si)).astype(jnp.bfloat16)
        wi = (factor * (im * co - re * si)).astype(jnp.bfloat16)
        acc = acc + wv * (re * re + im * im)
        prf = whole(q_s, real)
        pif = whole(q_s, imag)
        pr = prf.astype(jnp.bfloat16)
        pi = pif.astype(jnp.bfloat16)
        own = (jnp.where(first, wr, pr), jnp.where(first, wi, pi))
        other = (jnp.where(first, pr, wr), jnp.where(first, pi, wi))
        put(c == h, place, own, other)
        mag_s[:, sl] = prf * prf + pif * pif
    energy[...] = jnp.broadcast_to(jnp.sum(acc, axis=1, keepdims=True), (n, META))
    power = lax.dot_general(
        mag_s[...], wc2_s[...], NT_DIMS, precision=lax.Precision.HIGHEST, preferred_element_type=jnp.float32
    )
    lane = lax.broadcasted_iota(jnp.int32, (NBIN, META), 1)
    row = lax.broadcasted_iota(jnp.int32, (NBIN, META), 0)
    placed = jnp.zeros((n, META), jnp.float32)
    for k, part in enumerate(split3(power)):
        spot = jnp.where(lane == row + k * NBIN, 1.0, 0.0).astype(jnp.bfloat16)
        placed = placed + jnp.dot(part, spot, preferred_element_type=jnp.float32)
    tail = pl.ds(width, META)
    placed = placed.astype(jnp.bfloat16)
    own = jnp.where(first, meta[...], placed)
    other = jnp.where(first, placed, meta[...])
    own_a[:, tail] = own
    own_b[:, tail] = own
    send[0:n, tail] = other
    send[n : 2 * n, tail] = other


def prepare(c, x, q, w, ctf, binc, cx, sx, cy, sy, meta):
    n = x.shape[0] // 2
    width = x.shape[1]
    vm = pl.BlockSpec(memory_space=pltpu.VMEM)
    return pl.pallas_call(
        prep_kernel,
        out_shape=(
            jax.ShapeDtypeStruct((n, width + META), jnp.bfloat16),
            jax.ShapeDtypeStruct((n, width + META), jnp.bfloat16),
            jax.ShapeDtypeStruct((2 * n, width + META), jnp.bfloat16),
            jax.ShapeDtypeStruct((n, META), jnp.float32),
        ),
        in_specs=[pl.BlockSpec(memory_space=pltpu.SMEM)] + [vm] * 10,
        out_specs=(vm, vm, vm, vm),
        scratch_shapes=[
            pltpu.VMEM((NBIN, width), jnp.float32),
            pltpu.VMEM((n, width), jnp.float32),
            pltpu.VMEM((2, 2, 2 * n, BOX // 2), jnp.float32),
            pltpu.VMEM((2, 2, 2 * n, BOX // 2), jnp.float32),
        ],
        name="prep",
    )(c, x, q, w, ctf, binc, cx, sx, cy, sy, meta)


def score_kernel(n_pos, ids, *refs):
    it = iter(refs)
    take = lambda n: [next(it) for _ in range(n)]
    mine = take(n_pos)
    theirs = take(n_pos)
    mine_next = take(2)
    theirs_next = take(2)
    tables, tables_next = take(2)
    mine_meta = take(n_pos)
    theirs_meta = take(n_pos)
    out, part_s, proj_s, tab_s, rot_s, acc, w_s, pick_s, slot_s, label_s = take(10)
    step = pl.program_id(0)
    steps = pl.num_programs(0)
    rows = mine[0].shape[0]
    piece = rows // 2
    n_y = n_z = n_pos
    turns = 2 * n_z // TURN
    np_ = n_y * rows
    offs_y = ring_offsets(n_y)
    offs_z = ring_offsets(n_z)
    my_y = ids[0]
    my_z = ids[1]
    my_c = ids[2]

    def spread(y_refs, z_refs, z_later):
        at = 0
        for ref in y_refs:
            part_s[at : at + ref.shape[0], :] = ref[...]
            at += ref.shape[0]
        at = 0
        for ref in list(z_refs) + list(z_later):
            for i in range(ref.shape[0] // piece):
                tile = at // piece + i
                lo = tile % TURN * piece
                if tile // TURN <= turns:
                    proj_s[tile // TURN, lo : lo + piece, :] = ref[i * piece : (i + 1) * piece, :]
            at += ref.shape[0]

    @pl.when(my_c == 0)
    def _():
        spread(mine, theirs, theirs_next)

    @pl.when(my_c != 0)
    def _():
        spread(theirs, mine, mine_next)

    tab_s[0] = tables[...]
    tab_s[1] = tables_next[...]

    def rotate(b, slot, later):
        for s in range(TURN * piece // 16):
            sl = slice(s * 16, s * 16 + 16)
            i = s * 16 // piece
            at = s * 16 % piece
            for q in range(CHUNK // 256):
                la = slice(q * 256, q * 256 + 256)
                lb = slice(CHUNK + q * 256, CHUNK + q * 256 + 256)
                reb = proj_s[b, sl, la]
                imb = proj_s[b, sl, lb]
                re = reb.astype(jnp.float32)
                im = imb.astype(jnp.float32)
                base = (i * NT + 4) * piece + at
                rot_s[slot, base : base + 16, la] = reb
                rot_s[slot, base : base + 16, lb] = imb
                for k, (t1, t2, _, _) in enumerate(PAIRS):
                    co = tab_s[later, k : k + 1, la]
                    si = tab_s[later, 4 + k : 5 + k, la]
                    rc = re * co
                    is_ = im * si
                    ic = im * co
                    rs = re * si
                    b1 = (i * NT + t1) * piece + at
                    b2 = (i * NT + t2) * piece + at
                    rot_s[slot, b1 : b1 + 16, la] = (rc - is_).astype(jnp.bfloat16)
                    rot_s[slot, b1 : b1 + 16, lb] = (ic + rs).astype(jnp.bfloat16)
                    rot_s[slot, b2 : b2 + 16, la] = (rc + is_).astype(jnp.bfloat16)
                    rot_s[slot, b2 : b2 + 16, lb] = (ic - rs).astype(jnp.bfloat16)

    def window_slots(info):
        lane = lax.broadcasted_iota(jnp.int32, (1, np_), 1)
        slots = []
        for j in range(4):
            key = info[j : j + 1, :]
            local = key // 2 - my_y * 2 * n_z
            k_of = jnp.full((1, np_), -1, jnp.int32)
            for k in range(n_z):
                z_abs = (my_z - offs_z[k] + n_z) % n_z
                k_of = jnp.where((local >= 0) & (local // 2 == z_abs), k, k_of)
            slot = k_of * rows + (1 - local % 2) * piece + (lane // piece) * 2 + key % 2
            slots.append(jnp.where(k_of >= 0, slot, -1))
        return slots

    @pl.when(step == 0)
    def _():
        acc[...] = jnp.zeros_like(acc)
        rotate(0, 0, 0)
        a_meta = jnp.concatenate([m[...] for m in mine_meta], axis=0)
        b_meta = jnp.concatenate([m[...] for m in theirs_meta], axis=0)
        info_f = jnp.transpose(jnp.where(my_c == 0, a_meta, b_meta).astype(jnp.float32))
        info = info_f.astype(jnp.int32)
        slot_row = lax.broadcasted_iota(jnp.int32, (np_, np_), 0)
        which = lax.broadcasted_iota(jnp.int32, (8, np_), 0)
        total = jnp.zeros((np_, np_), jnp.float32)
        labels = jnp.zeros((8, np_), jnp.float32)
        for j, slot in enumerate(window_slots(info)):
            hit = jnp.where(slot_row == slot, 1.0, 0.0)
            total = total + hit
            values = jnp.where(which == 0, info_f[4 + j : 5 + j, :], info_f[8:9, :])
            labels = labels + lax.dot_general(
                values.astype(jnp.bfloat16),
                hit.astype(jnp.bfloat16),
                NT_DIMS,
                preferred_element_type=jnp.float32,
            )
        pick_s[...] = total.astype(jnp.bfloat16)
        label_s[...] = labels.astype(jnp.int32)

    for g in range(2):
        for q in range(4):
            la = slice(q * CHUNK // 2, (q + 1) * CHUNK // 2)
            slot_s[g, :, la] = jnp.dot(
                pick_s[g * np_ // 2 : (g + 1) * np_ // 2, :], part_s[:, la], preferred_element_type=jnp.float32
            ).astype(jnp.bfloat16)

    def body(b, carry):
        rotate(b + 1, (b + 1) % 2, jnp.where(b + 1 == turns, 1, 0))
        scored = lax.dot_general(
            rot_s[b % 2], slot_s[b // (turns // 2)], NT_DIMS, preferred_element_type=jnp.float32
        )
        for i in range(TURN):
            acc[b * TURN + i] += scored[i * NT * piece : (i + 1) * NT * piece]
        return carry

    lax.fori_loop(0, turns, body, 0)

    @pl.when(step == steps - 1)
    def _():
        a_meta = jnp.concatenate([m[...] for m in mine_meta], axis=0)
        b_meta = jnp.concatenate([m[...] for m in theirs_meta], axis=0)
        power_parts = jnp.where(my_c == 0, b_meta, a_meta)
        starts = label_s[0:1, :]
        bins = label_s[1:2, :]
        r = lax.broadcasted_iota(jnp.int32, (META, np_), 0)
        spot = jnp.where((r % NBIN == bins) & (r < 3 * NBIN), -0.25, 0.0).astype(jnp.bfloat16)
        power = jnp.dot(power_parts, spot, preferred_element_type=jnp.float32)
        section = lax.broadcasted_iota(jnp.int32, (1, 128), 1) // piece
        for lt in range(np_ // 128):
            la = slice(lt * 128, lt * 128 + 128)
            lo = lt % 2 * 128
            start = starts[:, la]
            tiles = [(2 * lt + i // 2, i % 2) for i in range(4)]
            level = jnp.zeros((piece, 128), jnp.float32)
            for i, (k, u) in enumerate(tiles):
                first = k * rows + u * piece
                level = jnp.where(section == i, power[first : first + piece, la], level)
            for t in range(NT):
                x = jnp.zeros((piece, 128), jnp.float32)
                for i, (k, u) in enumerate(tiles):
                    first = t * piece
                    x = jnp.where(section == i, acc[2 * k + u, first : first + piece, lo : lo + 128], x)
                x = x + level
                for bit in (16, 8, 4, 2, 1):
                    x = jnp.where((start & bit) != 0, pltpu.roll(x, piece - bit, 0), x)
                w_s[t * 16 : t * 16 + 16, la] = x[0:16]
        lane = lax.broadcasted_iota(jnp.int32, (1, np_), 1)
        z_of = jnp.zeros((1, np_), jnp.int32)
        y_of = jnp.zeros((1, np_), jnp.int32)
        block = lane % piece // 2
        for k in range(n_pos):
            z_of = jnp.where(lane // rows == k, (my_z - offs_z[k] + n_z) % n_z, z_of)
            y_of = jnp.where(block // 2 == k, (my_y - offs_y[k] + n_y) % n_y, y_of)
        tile = z_of * 2 + 1 - lane // piece % 2
        place = (y_of * 2 + block % 2) * 4 * n_z + tile * 2 + lane % 2
        slot_row = lax.broadcasted_iota(jnp.int32, (out.shape[0], np_), 0)
        moved = jnp.where(slot_row == place, 1.0, 0.0).astype(jnp.bfloat16)
        total = jnp.zeros(out.shape, jnp.float32)
        for part in split3(w_s[...]):
            total = total + lax.dot_general(moved, part, NT_DIMS, preferred_element_type=jnp.float32)
        out[...] = total


def score(ids, mine, theirs, tables):
    n_pos = len(mine)
    rows = mine[0].shape[0]
    piece = rows // 2
    width = mine[0].shape[1] - META
    span = 2 * CHUNK
    steps = width // span
    n_slots = 2 * n_pos * 4 * n_pos
    np_ = n_pos * rows
    after = lambda i, s: (0, jnp.minimum(i + 1, steps - 1))
    now = [pl.BlockSpec((a.shape[0], span), lambda i, s: (0, i)) for a in mine]
    later = pl.BlockSpec((rows, span), after)
    table = pl.BlockSpec((8, CHUNK), lambda i, s: (0, i))
    table_later = pl.BlockSpec((8, CHUNK), after)
    tail = [pl.BlockSpec((a.shape[0], META), lambda i, s: (0, width // META)) for a in mine]
    flops = (NT + 1) * np_ * np_ * width
    return pl.pallas_call(
        functools.partial(score_kernel, n_pos),
        out_shape=jax.ShapeDtypeStruct((n_slots, NT * 16), jnp.float32),
        grid_spec=pltpu.PrefetchScalarGridSpec(
            num_scalar_prefetch=1,
            grid=(steps,),
            in_specs=now + now + [later] * 4 + [table, table_later] + tail + tail,
            out_specs=pl.BlockSpec((n_slots, NT * 16), lambda i, s: (0, 0)),
            scratch_shapes=[
                pltpu.VMEM((np_, span), jnp.bfloat16),
                pltpu.VMEM((2 * n_pos // TURN + 1, TURN * piece, span), jnp.bfloat16),
                pltpu.VMEM((2, 8, CHUNK), jnp.float32),
                pltpu.VMEM((2, NT * TURN * piece, span), jnp.bfloat16),
                pltpu.VMEM((2 * n_pos, NT * piece, np_ // 2), jnp.float32),
                pltpu.VMEM((NT * 16, np_), jnp.float32),
                pltpu.VMEM((np_, np_), jnp.bfloat16),
                pltpu.VMEM((2, np_ // 2, span), jnp.bfloat16),
                pltpu.VMEM((8, np_), jnp.int32),
            ],
        ),
        compiler_params=pltpu.CompilerParams(
            dimension_semantics=("arbitrary",),
            vmem_limit_bytes=60 * 1024 * 1024,
        ),
        cost_estimate=pl.CostEstimate(flops=flops, transcendentals=0, bytes_accessed=17 * 1024 * 1024),
        name="score",
    )(ids, *mine, *theirs, *mine[:2], *theirs[:2], tables, tables, *mine, *theirs)


def core_rings(first, second, n):
    spot = lambda y, z, c: (y % n * n + z % n) * 2 + c
    cells = [(y, z) for y in range(n) for z in range(n)]

    def shift(v, d):
        pairs = [(spot(y, z, 0), spot(y + d, z, 0)) for y, z in cells]
        pairs += [(spot(y, z, 1), spot(y, z + d, 1)) for y, z in cells]
        return lax.ppermute(v, TILE, pairs)

    def swap(v):
        return lax.ppermute(v, TILE[2], [(0, 1), (1, 0)])

    ahead = [first, second]
    back = [first, second]
    theirs, mine = [swap(first)], [second]
    for s in range(1, n // 2 + 1):
        for k in range(2):
            if s < n // 2:
                ahead[k] = shift(ahead[k], 1)
                back[k] = shift(back[k], -1)
                new = [ahead[k], back[k]]
            else:
                new = [shift(ahead[k], 1) if k == 0 else shift(back[k], -1)]
            if k == 0:
                theirs += [swap(v) for v in new]
            else:
                mine += new
    return mine, theirs


def slot_rank(tile_ids):
    positions = jnp.arange(tile_ids.shape[0], dtype=jnp.int32)
    earlier_same = (tile_ids[:, None] == tile_ids[None, :]) & (
        positions[None, :] < positions[:, None]
    )
    return jnp.sum(earlier_same.astype(jnp.int32), axis=1)


def finish(scored):
    row_peak = jnp.max(scored, axis=(1, 2))
    log_total = row_peak + jnp.log(jnp.sum(jnp.exp(scored - row_peak[:, None, None]), axis=(1, 2)))
    posterior = jnp.exp(scored - log_total[:, None, None])
    return (posterior, log_total)


def per_device(particles, projections, noise_weight, tile_list, ori_start, shifts, defocus_bin):
    band = lax.axis_index("shell")
    my_y = lax.axis_index(TILE[0])
    my_z = lax.axis_index(TILE[1])
    my_c = lax.axis_index(TILE[2])
    count, _, width = particles.shape
    windows = tile_list.shape[1]
    half = width // 2
    freq_x, freq_y = frequencies(band * width, width)
    ctf = ctf_table(freq_x, freq_y, NBIN)
    first_x = (band * width) // BOX
    span_x = first_x + jnp.arange(width // BOX, dtype=jnp.int32)
    span_y = jnp.arange(BOX, dtype=jnp.int32) - BOX // 2
    cx, sx = turn(span_x[None, :] * shifts[:, 0:1])
    cy, sy = turn(span_y[None, :] * shifts[:, 1:2])
    key = tile_list * 2 + slot_rank(tile_list.reshape(-1)).reshape(count, windows)
    meta = jnp.concatenate([key, ori_start, defocus_bin[:, None]], axis=1)
    meta = jnp.pad(meta, ((0, 0), (0, META - meta.shape[1]))).astype(jnp.bfloat16)
    own_a, own_b, send, energy = prepare(
        my_c.reshape(1).astype(jnp.int32),
        particles.reshape(2 * count, width),
        projections.reshape(2 * count, width),
        noise_weight[None, :],
        ctf,
        defocus_bin[:, None],
        cx,
        sx,
        cy,
        sy,
        meta,
    )
    got = lax.ppermute(send, TILE[2], [(0, 1), (1, 0)])
    kept = jnp.concatenate([own_a, got[:count]], axis=0)
    passed = jnp.concatenate([own_b, got[count:]], axis=0)
    mine, theirs = core_rings(passed, kept, lax.axis_size(TILE[0]))
    mult = jnp.array([[a, b] for _, _, a, b in PAIRS], jnp.int32)
    fx = lax.dynamic_slice_in_dim(freq_x, my_c * half, half)
    fy = lax.dynamic_slice_in_dim(freq_y, my_c * half, half)
    co, si = turn(mult[:, 0:1] * fx[None, :] + mult[:, 1:2] * fy[None, :])
    tables = jnp.concatenate([co, si], axis=0)
    ids = jnp.stack([my_y, my_z, my_c]).astype(jnp.int32)
    slots = score(ids, mine, theirs, tables)
    n_y = lax.axis_size(TILE[0])
    slots = slots.reshape(2 * n_y, -1, NT * 16)
    slots = lax.all_to_all(slots, (TILE[0], TILE[2]), split_axis=0, concat_axis=0, tiled=True)
    slots = jnp.sum(slots.reshape(n_y, 2, -1, NT * 16), axis=1).reshape(-1, NT * 16)
    items = jnp.take(slots, key.reshape(-1), axis=0)
    items = items.reshape(count, windows * NT * 16) - 0.5 * energy[:, 0:1]
    n_x = lax.axis_size("shell")
    copies = jnp.broadcast_to(items, (n_x, *items.shape))
    items = jnp.sum(lax.all_to_all(copies, "shell", split_axis=0, concat_axis=0, tiled=True), axis=0)
    scores = items.reshape(count, windows, NT, 16).transpose(0, 2, 1, 3).reshape(count, NT, windows * 16)
    return finish(scores)


def solution(mesh):
    split = Mesh(
        mesh.devices.reshape(8, 8, 2, mesh.shape["shell"]), ("tile_0", "tile_1", "tile_2", "shell")
    )
    in_specs = (
        P(TILE, None, "shell"),
        P(TILE, None, "shell"),
        P("shell"),
        P(TILE, None),
        P(TILE, None),
        P(TILE, None),
        P(TILE),
    )
    out_specs = (P(TILE, None, None), P(TILE))
    return jax.shard_map(
        per_device, mesh=split, in_specs=in_specs, out_specs=out_specs, check_vma=False
    )
```

```python
import functools
import math

import jax
import jax.numpy as jnp
from jax import lax
from jax.experimental import pallas as pl
from jax.experimental.pallas import tpu as pltpu
from jax.sharding import Mesh
from jax.sharding import PartitionSpec as P

BOX = 256
NBIN = 16
TSIDE = 3
NT = TSIDE * TSIDE
TILE = ("tile_0", "tile_1", "tile_2")

wave_length = 0.0197
aberration = 27000000.0
amplitude = 0.1
b_factor = 20.0
defocus_base = 5000.0
defocus_step = 500.0

META = 128
TURN = 2
CHUNK = 1024
PAIRS = ((5, 3, 0, 1), (7, 1, 1, 0), (8, 0, 1, 1), (6, 2, 1, -1))


def ring_offsets(n):
    offs = [0]
    for s in range(1, n // 2):
        offs += [s, -s]
    return offs + [n // 2]


def frequencies(first_index, span_count):
    flat_index = first_index + jnp.arange(span_count, dtype=jnp.int32)
    freq_x = flat_index // BOX
    freq_y = flat_index % BOX - BOX // 2
    return (freq_x, freq_y)


def ctf_table(freq_x, freq_y, bins_count):
    scaled_x = freq_x.astype(jnp.float32) / BOX
    scaled_y = freq_y.astype(jnp.float32) / BOX
    radius_sq = scaled_x * scaled_x + scaled_y * scaled_y
    defocus = defocus_base + defocus_step * jnp.arange(bins_count, dtype=jnp.float32)[:, None]
    aberr_phase = (
        math.pi * wave_length * defocus * radius_sq[None, :]
        - 0.5 * math.pi * aberration * wave_length**3 * radius_sq[None, :] ** 2
    )
    envelope = jnp.exp(-0.25 * b_factor * radius_sq)[None, :]
    return (
        -(math.sqrt(1.0 - amplitude**2) * jnp.sin(aberr_phase) + amplitude * jnp.cos(aberr_phase))
        * envelope
    )


def turn(m):
    angles = jnp.mod(m, BOX).astype(jnp.float32) * (2.0 * math.pi / BOX)
    return (jnp.cos(angles), jnp.sin(angles))


def split3(v):
    hi = v.astype(jnp.bfloat16)
    rest = v - hi.astype(jnp.float32)
    mid = rest.astype(jnp.bfloat16)
    lo = (rest - mid.astype(jnp.float32)).astype(jnp.bfloat16)
    return hi, mid, lo


NT_DIMS = (((1,), (1,)), ((), ()))


def prep_kernel(
    c_ref, x, q, w, ctf, cx, sx, cy, sy, meta, own_a, own_b, send, energy, wc2_s, mag_s, x_s, q_s
):
    n = x.shape[0] // 2
    width = x.shape[1]
    real = pl.ds(0, n, stride=2)
    imag = pl.ds(1, n, stride=2)
    half = width // 2
    c = c_ref[0]
    bins = meta[...].astype(jnp.float32)[:, 8:9].astype(jnp.int32)
    acc = jnp.zeros((n, BOX), jnp.float32)
    cyv = cy[...]
    syv = sy[...]

    first = c == 0

    def put(mine, place, own, other):
        for k in range(2):
            a = pl.ds(place + k * CHUNK, BOX)

            @pl.when(mine)
            def _(k=k, a=a):
                own_a[:, a] = own[k]
                send[n : 2 * n, a] = other[k]

            @pl.when(jnp.logical_not(mine))
            def _(k=k, a=a):
                own_b[:, a] = own[k]
                send[0:n, a] = other[k]

    for g in range(width // BOX):
        sl = pl.ds(g * BOX, BOX)
        wv = w[:, sl]
        table = ctf[:, sl]
        wc2_s[:, sl] = wv * table * table
        rows = jnp.zeros((n, BOX), jnp.float32)
        for b in range(NBIN):
            rows = jnp.where(bins == b, table[b : b + 1, :], rows)
        x_s[g % 2, 0] = x[:, pl.ds(g * BOX, BOX // 2)].astype(jnp.float32)
        x_s[g % 2, 1] = x[:, pl.ds(g * BOX + BOX // 2, BOX // 2)].astype(jnp.float32)
        q_s[g % 2, 0] = q[:, pl.ds(g * BOX, BOX // 2)].astype(jnp.float32)
        q_s[g % 2, 1] = q[:, pl.ds(g * BOX + BOX // 2, BOX // 2)].astype(jnp.float32)
        whole = lambda ref, part: jnp.concatenate([ref[g % 2, i, part, :] for i in range(2)], axis=1)
        re = whole(x_s, real)
        im = whole(x_s, imag)
        cxv = cx[:, g : g + 1]
        sxv = sx[:, g : g + 1]
        co = cxv * cyv - sxv * syv
        si = sxv * cyv + cxv * syv
        factor = wv * rows
        h = (g * BOX) // half
        at = g * BOX - h * half
        place = (at // CHUNK) * 2 * CHUNK + at % CHUNK
        wr = (factor * (re * co + im * si)).astype(jnp.bfloat16)
        wi = (factor * (im * co - re * si)).astype(jnp.bfloat16)
        acc = acc + wv * (re * re + im * im)
        prf = whole(q_s, real)
        pif = whole(q_s, imag)
        pr = prf.astype(jnp.bfloat16)
        pi = pif.astype(jnp.bfloat16)
        own = (jnp.where(first, wr, pr), jnp.where(first, wi, pi))
        other = (jnp.where(first, pr, wr), jnp.where(first, pi, wi))
        put(c == h, place, own, other)
        mag_s[:, sl] = prf * prf + pif * pif
    energy[...] = jnp.broadcast_to(jnp.sum(acc, axis=1, keepdims=True), (n, META))
    power = lax.dot_general(
        mag_s[...], wc2_s[...], NT_DIMS, precision=lax.Precision.HIGHEST, preferred_element_type=jnp.float32
    )
    lane = lax.broadcasted_iota(jnp.int32, (NBIN, META), 1)
    row = lax.broadcasted_iota(jnp.int32, (NBIN, META), 0)
    placed = jnp.zeros((n, META), jnp.float32)
    for k, part in enumerate(split3(power)):
        spot = jnp.where(lane == row + k * NBIN, 1.0, 0.0).astype(jnp.bfloat16)
        placed = placed + jnp.dot(part, spot, preferred_element_type=jnp.float32)
    tail = pl.ds(width, META)
    placed = placed.astype(jnp.bfloat16)
    own = jnp.where(first, meta[...], placed)
    other = jnp.where(first, placed, meta[...])
    own_a[:, tail] = own
    own_b[:, tail] = own
    send[0:n, tail] = other
    send[n : 2 * n, tail] = other


def prepare(c, x, q, w, ctf, cx, sx, cy, sy, meta):
    n = x.shape[0] // 2
    width = x.shape[1]
    vm = pl.BlockSpec(memory_space=pltpu.VMEM)
    return pl.pallas_call(
        prep_kernel,
        out_shape=(
            jax.ShapeDtypeStruct((n, width + META), jnp.bfloat16),
            jax.ShapeDtypeStruct((n, width + META), jnp.bfloat16),
            jax.ShapeDtypeStruct((2 * n, width + META), jnp.bfloat16),
            jax.ShapeDtypeStruct((n, META), jnp.float32),
        ),
        in_specs=[pl.BlockSpec(memory_space=pltpu.SMEM)] + [vm] * 9,
        out_specs=(vm, vm, vm, vm),
        scratch_shapes=[
            pltpu.VMEM((NBIN, width), jnp.float32),
            pltpu.VMEM((n, width), jnp.float32),
            pltpu.VMEM((2, 2, 2 * n, BOX // 2), jnp.float32),
            pltpu.VMEM((2, 2, 2 * n, BOX // 2), jnp.float32),
        ],
        name="prep",
    )(c, x, q, w, ctf, cx, sx, cy, sy, meta)


def score_kernel(n_pos, ids, *refs):
    it = iter(refs)
    take = lambda n: [next(it) for _ in range(n)]
    mine = take(n_pos)
    theirs = take(n_pos)
    mine_next = take(2)
    theirs_next = take(2)
    tables, tables_next = take(2)
    mine_meta = take(n_pos)
    theirs_meta = take(n_pos)
    out, part_s, proj_s, tab_s, rot_s, acc, w_s, pick_s, slot_s, label_s = take(10)
    step = pl.program_id(0)
    steps = pl.num_programs(0)
    rows = mine[0].shape[0]
    piece = rows // 2
    n_y = n_z = n_pos
    turns = 2 * n_z // TURN
    np_ = n_y * rows
    offs_y = ring_offsets(n_y)
    offs_z = ring_offsets(n_z)
    my_y = ids[0]
    my_z = ids[1]
    my_c = ids[2]

    def spread(y_refs, z_refs, z_later):
        at = 0
        for ref in y_refs:
            part_s[at : at + ref.shape[0], :] = ref[...]
            at += ref.shape[0]
        at = 0
        for ref in list(z_refs) + list(z_later):
            for i in range(ref.shape[0] // piece):
                tile = at // piece + i
                lo = tile % TURN * piece
                if tile // TURN <= turns:
                    proj_s[tile // TURN, lo : lo + piece, :] = ref[i * piece : (i + 1) * piece, :]
            at += ref.shape[0]

    @pl.when(my_c == 0)
    def _():
        spread(mine, theirs, theirs_next)

    @pl.when(my_c != 0)
    def _():
        spread(theirs, mine, mine_next)

    tab_s[0] = tables[...]
    tab_s[1] = tables_next[...]

    def rotate(b, slot, later):
        for s in range(TURN * piece // 16):
            sl = slice(s * 16, s * 16 + 16)
            i = s * 16 // piece
            at = s * 16 % piece
            for q in range(CHUNK // 256):
                la = slice(q * 256, q * 256 + 256)
                lb = slice(CHUNK + q * 256, CHUNK + q * 256 + 256)
                reb = proj_s[b, sl, la]
                imb = proj_s[b, sl, lb]
                re = reb.astype(jnp.float32)
                im = imb.astype(jnp.float32)
                base = (i * NT + 4) * piece + at
                rot_s[slot, base : base + 16, la] = reb
                rot_s[slot, base : base + 16, lb] = imb
                for k, (t1, t2, _, _) in enumerate(PAIRS):
                    co = tab_s[later, k : k + 1, la]
                    si = tab_s[later, 4 + k : 5 + k, la]
                    rc = re * co
                    is_ = im * si
                    ic = im * co
                    rs = re * si
                    b1 = (i * NT + t1) * piece + at
                    b2 = (i * NT + t2) * piece + at
                    rot_s[slot, b1 : b1 + 16, la] = (rc - is_).astype(jnp.bfloat16)
                    rot_s[slot, b1 : b1 + 16, lb] = (ic + rs).astype(jnp.bfloat16)
                    rot_s[slot, b2 : b2 + 16, la] = (rc + is_).astype(jnp.bfloat16)
                    rot_s[slot, b2 : b2 + 16, lb] = (ic - rs).astype(jnp.bfloat16)

    def window_slots(info):
        lane = lax.broadcasted_iota(jnp.int32, (1, np_), 1)
        slots = []
        for j in range(4):
            key = info[j : j + 1, :]
            local = key // 2 - my_y * 2 * n_z
            k_of = jnp.full((1, np_), -1, jnp.int32)
            for k in range(n_z):
                z_abs = (my_z - offs_z[k] + n_z) % n_z
                k_of = jnp.where((local >= 0) & (local // 2 == z_abs), k, k_of)
            slot = k_of * rows + (1 - local % 2) * piece + (lane // piece) * 2 + key % 2
            slots.append(jnp.where(k_of >= 0, slot, -1))
        return slots

    @pl.when(step == 0)
    def _():
        acc[...] = jnp.zeros_like(acc)
        rotate(0, 0, 0)
        a_meta = jnp.concatenate([m[...] for m in mine_meta], axis=0)
        b_meta = jnp.concatenate([m[...] for m in theirs_meta], axis=0)
        info_f = jnp.transpose(jnp.where(my_c == 0, a_meta, b_meta).astype(jnp.float32))
        info = info_f.astype(jnp.int32)
        slot_row = lax.broadcasted_iota(jnp.int32, (np_, np_), 0)
        which = lax.broadcasted_iota(jnp.int32, (8, np_), 0)
        total = jnp.zeros((np_, np_), jnp.float32)
        labels = jnp.zeros((8, np_), jnp.float32)
        for j, slot in enumerate(window_slots(info)):
            hit = jnp.where(slot_row == slot, 1.0, 0.0)
            total = total + hit
            values = jnp.where(which == 0, info_f[4 + j : 5 + j, :], info_f[8:9, :])
            labels = labels + lax.dot_general(
                values.astype(jnp.bfloat16),
                hit.astype(jnp.bfloat16),
                NT_DIMS,
                preferred_element_type=jnp.float32,
            )
        pick_s[...] = total.astype(jnp.bfloat16)
        label_s[...] = labels.astype(jnp.int32)

    for g in range(2):
        for q in range(4):
            la = slice(q * CHUNK // 2, (q + 1) * CHUNK // 2)
            slot_s[g, :, la] = jnp.dot(
                pick_s[g * np_ // 2 : (g + 1) * np_ // 2, :], part_s[:, la], preferred_element_type=jnp.float32
            ).astype(jnp.bfloat16)

    def body(b, carry):
        rotate(b + 1, (b + 1) % 2, jnp.where(b + 1 == turns, 1, 0))
        scored = lax.dot_general(
            rot_s[b % 2], slot_s[b // (turns // 2)], NT_DIMS, preferred_element_type=jnp.float32
        )
        for i in range(TURN):
            acc[b * TURN + i] += scored[i * NT * piece : (i + 1) * NT * piece]
        return carry

    lax.fori_loop(0, turns, body, 0)

    @pl.when(step == steps - 1)
    def _():
        a_meta = jnp.concatenate([m[...] for m in mine_meta], axis=0)
        b_meta = jnp.concatenate([m[...] for m in theirs_meta], axis=0)
        power_parts = jnp.where(my_c == 0, b_meta, a_meta)
        starts = label_s[0:1, :]
        bins = label_s[1:2, :]
        r = lax.broadcasted_iota(jnp.int32, (META, np_), 0)
        spot = jnp.where((r % NBIN == bins) & (r < 3 * NBIN), -0.25, 0.0).astype(jnp.bfloat16)
        power = jnp.dot(power_parts, spot, preferred_element_type=jnp.float32)
        section = lax.broadcasted_iota(jnp.int32, (1, 128), 1) // piece
        for lt in range(np_ // 128):
            la = slice(lt * 128, lt * 128 + 128)
            lo = lt % 2 * 128
            start = starts[:, la]
            tiles = [(2 * lt + i // 2, i % 2) for i in range(4)]
            level = jnp.zeros((piece, 128), jnp.float32)
            for i, (k, u) in enumerate(tiles):
                first = k * rows + u * piece
                level = jnp.where(section == i, power[first : first + piece, la], level)
            for t in range(NT):
                x = jnp.zeros((piece, 128), jnp.float32)
                for i, (k, u) in enumerate(tiles):
                    first = t * piece
                    x = jnp.where(section == i, acc[2 * k + u, first : first + piece, lo : lo + 128], x)
                x = x + level
                for bit in (16, 8, 4, 2, 1):
                    x = jnp.where((start & bit) != 0, pltpu.roll(x, piece - bit, 0), x)
                w_s[t * 16 : t * 16 + 16, la] = x[0:16]
        lane = lax.broadcasted_iota(jnp.int32, (1, np_), 1)
        z_of = jnp.zeros((1, np_), jnp.int32)
        y_of = jnp.zeros((1, np_), jnp.int32)
        block = lane % piece // 2
        for k in range(n_pos):
            z_of = jnp.where(lane // rows == k, (my_z - offs_z[k] + n_z) % n_z, z_of)
            y_of = jnp.where(block // 2 == k, (my_y - offs_y[k] + n_y) % n_y, y_of)
        tile = z_of * 2 + 1 - lane // piece % 2
        place = (y_of * 2 + block % 2) * 4 * n_z + tile * 2 + lane % 2
        slot_row = lax.broadcasted_iota(jnp.int32, (out.shape[0], np_), 0)
        moved = jnp.where(slot_row == place, 1.0, 0.0).astype(jnp.bfloat16)
        total = jnp.zeros(out.shape, jnp.float32)
        for part in split3(w_s[...]):
            total = total + lax.dot_general(moved, part, NT_DIMS, preferred_element_type=jnp.float32)
        out[...] = total


def score(ids, mine, theirs, tables):
    n_pos = len(mine)
    rows = mine[0].shape[0]
    piece = rows // 2
    width = mine[0].shape[1] - META
    span = 2 * CHUNK
    steps = width // span
    n_slots = 2 * n_pos * 4 * n_pos
    np_ = n_pos * rows
    after = lambda i, s: (0, jnp.minimum(i + 1, steps - 1))
    now = [pl.BlockSpec((a.shape[0], span), lambda i, s: (0, i)) for a in mine]
    later = pl.BlockSpec((rows, span), after)
    table = pl.BlockSpec((8, CHUNK), lambda i, s: (0, i))
    table_later = pl.BlockSpec((8, CHUNK), after)
    tail = [pl.BlockSpec((a.shape[0], META), lambda i, s: (0, width // META)) for a in mine]
    flops = (NT + 1) * np_ * np_ * width
    return pl.pallas_call(
        functools.partial(score_kernel, n_pos),
        out_shape=jax.ShapeDtypeStruct((n_slots, NT * 16), jnp.float32),
        grid_spec=pltpu.PrefetchScalarGridSpec(
            num_scalar_prefetch=1,
            grid=(steps,),
            in_specs=now + now + [later] * 4 + [table, table_later] + tail + tail,
            out_specs=pl.BlockSpec((n_slots, NT * 16), lambda i, s: (0, 0)),
            scratch_shapes=[
                pltpu.VMEM((np_, span), jnp.bfloat16),
                pltpu.VMEM((2 * n_pos // TURN + 1, TURN * piece, span), jnp.bfloat16),
                pltpu.VMEM((2, 8, CHUNK), jnp.float32),
                pltpu.VMEM((2, NT * TURN * piece, span), jnp.bfloat16),
                pltpu.VMEM((2 * n_pos, NT * piece, np_ // 2), jnp.float32),
                pltpu.VMEM((NT * 16, np_), jnp.float32),
                pltpu.VMEM((np_, np_), jnp.bfloat16),
                pltpu.VMEM((2, np_ // 2, span), jnp.bfloat16),
                pltpu.VMEM((8, np_), jnp.int32),
            ],
        ),
        compiler_params=pltpu.CompilerParams(
            dimension_semantics=("arbitrary",),
            vmem_limit_bytes=60 * 1024 * 1024,
        ),
        cost_estimate=pl.CostEstimate(flops=flops, transcendentals=0, bytes_accessed=17 * 1024 * 1024),
        name="score",
    )(ids, *mine, *theirs, *mine[:2], *theirs[:2], tables, tables, *mine, *theirs)


def core_rings(first, second, n):
    spot = lambda y, z, c: (y % n * n + z % n) * 2 + c
    cells = [(y, z) for y in range(n) for z in range(n)]

    def shift(v, d):
        pairs = [(spot(y, z, 0), spot(y + d, z, 0)) for y, z in cells]
        pairs += [(spot(y, z, 1), spot(y, z + d, 1)) for y, z in cells]
        return lax.ppermute(v, TILE, pairs)

    def swap(v):
        return lax.ppermute(v, TILE[2], [(0, 1), (1, 0)])

    ahead = [first, second]
    back = [first, second]
    theirs, mine = [swap(first)], [second]
    for s in range(1, n // 2 + 1):
        for k in range(2):
            if s < n // 2:
                ahead[k] = shift(ahead[k], 1)
                back[k] = shift(back[k], -1)
                new = [ahead[k], back[k]]
            else:
                new = [shift(ahead[k], 1) if k == 0 else shift(back[k], -1)]
            if k == 0:
                theirs += [swap(v) for v in new]
            else:
                mine += new
    return mine, theirs


def slot_rank(tile_ids):
    positions = jnp.arange(tile_ids.shape[0], dtype=jnp.int32)
    earlier_same = (tile_ids[:, None] == tile_ids[None, :]) & (
        positions[None, :] < positions[:, None]
    )
    return jnp.sum(earlier_same.astype(jnp.int32), axis=1)


def finish(scored):
    row_peak = jnp.max(scored, axis=(1, 2))
    log_total = row_peak + jnp.log(jnp.sum(jnp.exp(scored - row_peak[:, None, None]), axis=(1, 2)))
    posterior = jnp.exp(scored - log_total[:, None, None])
    return (posterior, log_total)


def per_device(particles, projections, noise_weight, tile_list, ori_start, shifts, defocus_bin):
    band = lax.axis_index("shell")
    my_y = lax.axis_index(TILE[0])
    my_z = lax.axis_index(TILE[1])
    my_c = lax.axis_index(TILE[2])
    count, _, width = particles.shape
    windows = tile_list.shape[1]
    half = width // 2
    freq_x, freq_y = frequencies(band * width, width)
    ctf = ctf_table(freq_x, freq_y, NBIN)
    first_x = (band * width) // BOX
    span_x = first_x + jnp.arange(width // BOX, dtype=jnp.int32)
    span_y = jnp.arange(BOX, dtype=jnp.int32) - BOX // 2
    cx, sx = turn(span_x[None, :] * shifts[:, 0:1])
    cy, sy = turn(span_y[None, :] * shifts[:, 1:2])
    key = tile_list * 2 + slot_rank(tile_list.reshape(-1)).reshape(count, windows)
    meta = jnp.concatenate([key, ori_start, defocus_bin[:, None]], axis=1)
    meta = jnp.pad(meta, ((0, 0), (0, META - meta.shape[1]))).astype(jnp.bfloat16)
    own_a, own_b, send, energy = prepare(
        my_c.reshape(1).astype(jnp.int32),
        particles.reshape(2 * count, width),
        projections.reshape(2 * count, width),
        noise_weight[None, :],
        ctf,
        cx,
        sx,
        cy,
        sy,
        meta,
    )
    got = lax.ppermute(send, TILE[2], [(0, 1), (1, 0)])
    kept = jnp.concatenate([own_a, got[:count]], axis=0)
    passed = jnp.concatenate([own_b, got[count:]], axis=0)
    mine, theirs = core_rings(passed, kept, lax.axis_size(TILE[0]))
    mult = jnp.array([[a, b] for _, _, a, b in PAIRS], jnp.int32)
    fx = lax.dynamic_slice_in_dim(freq_x, my_c * half, half)
    fy = lax.dynamic_slice_in_dim(freq_y, my_c * half, half)
    co, si = turn(mult[:, 0:1] * fx[None, :] + mult[:, 1:2] * fy[None, :])
    tables = jnp.concatenate([co, si], axis=0)
    ids = jnp.stack([my_y, my_z, my_c]).astype(jnp.int32)
    slots = score(ids, mine, theirs, tables)
    n_y = lax.axis_size(TILE[0])
    slots = slots.reshape(2 * n_y, -1, NT * 16)
    slots = lax.all_to_all(slots, (TILE[0], TILE[2]), split_axis=0, concat_axis=0, tiled=True)
    slots = jnp.sum(slots.reshape(n_y, 2, -1, NT * 16), axis=1).reshape(-1, NT * 16)
    items = jnp.take(slots, key.reshape(-1), axis=0)
    items = items.reshape(count, windows * NT * 16) - 0.5 * energy[:, 0:1]
    n_x = lax.axis_size("shell")
    copies = jnp.broadcast_to(items, (n_x, *items.shape))
    items = jnp.sum(lax.all_to_all(copies, "shell", split_axis=0, concat_axis=0, tiled=True), axis=0)
    scores = items.reshape(count, windows, NT, 16).transpose(0, 2, 1, 3).reshape(count, NT, windows * 16)
    return finish(scores)


def solution(mesh):
    split = Mesh(
        mesh.devices.reshape(8, 8, 2, mesh.shape["shell"]), ("tile_0", "tile_1", "tile_2", "shell")
    )
    in_specs = (
        P(TILE, None, "shell"),
        P(TILE, None, "shell"),
        P("shell"),
        P(TILE, None),
        P(TILE, None),
        P(TILE, None),
        P(TILE),
    )
    out_specs = (P(TILE, None, None), P(TILE))
    return jax.shard_map(
        per_device, mesh=split, in_specs=in_specs, out_specs=out_specs, check_vma=False
    )
```
